512 devices in a mesh: dom: 8 (over y, x_lo), energy: 64 (over x_hi, z, core).
Axes of the slice: x: 4 (x_hi: 2, x_lo: 2; x = x_hi * 2 + x_lo), y: 4, z: 16, core: 2. Of those that a mesh axis runs over, the one named last changes fastest.
Arguments:
- hamiltonian: float32 [8, 128, 128], P('dom'), may hold values from -0.5 to 0.5
- coupling: float32 [8, 64, 64], P('dom'), may hold values from -0.75 to 0.75
- contact_rates: float32 [2, 64], replicated, may hold values from 0.2 to 2
- occupation: float32 [1, 64, 2], P(None, 'energy'), may hold values from 0 to 1
- lesser_in: float32 [1, 64, 8, 2, 128, 128], P(None, 'energy', 'dom'), may hold values from -1 to 1, as said below
- greater_in: float32 [1, 64, 8, 2, 128, 128], P(None, 'energy', 'dom'), may hold values from -1 to 1, as said below
- phonon_shift: int32 [1], replicated, may hold values from 1 to 31
Outputs:
- lesser_out: float32 [1, 64, 8, 2, 128, 128], P(None, 'energy', 'dom')
- greater_out: float32 [1, 64, 8, 2, 128, 128], P(None, 'energy', 'dom')
The draws below stay inside these ranges and needn't reach their ends.
Inputs may be any that keep to these rules, and one draw needn't show every extreme that they name: Each block of lesser_in is i times a Hermitian positive semidefinite matrix. Each block of greater_in is -i times a Hermitian positive semidefinite matrix. phonon_shift is below 32.
All inputs are finite; a program needn't handle non-finite values.
Results may differ from the reference program's by a relative error of at most 0.00027.
Values sent between devices are 32-bit elements; how exact they have to be, the bound alone decides.
No kernel may reach another device: no remote copies, remote signals or barrier semaphores. Data moves between devices by JAX's collectives and lax.ppermute only.
A program may use at most 64 MiB of HBM per device.

```python
import math
import jax
import jax.numpy as jnp
from jax import lax

M = 128
INTERFACE = 64
E_DEV = 1
NB = 8
KMAX = 32
N_ENERGY = 64


def hermitian_blocks(key, sign_factor):
    block_count = E_DEV * N_ENERGY * NB
    key_level, key_real, key_imag = jax.random.split(key, 3)
    levels = jnp.exp(jax.random.uniform(key_level, (block_count, M), jnp.float32, 0.0, math.log(3.0)))
    spread = 0.05 / math.sqrt(M)
    raw_real = spread * jax.random.normal(key_real, (block_count, M, M), jnp.float32)
    raw_imag = spread * jax.random.normal(key_imag, (block_count, M, M), jnp.float32)
    sym_real = 0.5 * (raw_real + jnp.swapaxes(raw_real, 1, 2))
    skew_imag = 0.5 * (raw_imag - jnp.swapaxes(raw_imag, 1, 2))
    diagonal = 0.13 * levels[:, :, None] * jnp.eye(M, dtype=jnp.float32)
    positive_real = diagonal + sym_real
    positive_imag = skew_imag
    stacked = jnp.stack([-sign_factor * positive_imag, sign_factor * positive_real], 1)
    return stacked.reshape(E_DEV, N_ENERGY, NB, 2, M, M)


def draw_lesser_in(key, part):
    return hermitian_blocks(jax.random.fold_in(key, 11), 1.0)


def draw_greater_in(key, part):
    return hermitian_blocks(jax.random.fold_in(key, 23), -1.0)


def block_levels(stream_key, shape, cuts, least, largest):
    level, own = 1.0, jax.random.fold_in(stream_key, 6)
    for axis_at, parts in cuts:
        heights = jnp.exp(jax.random.uniform(jax.random.fold_in(own, axis_at), (parts,), jnp.float32, least / len(cuts), largest / len(cuts)))
        level = level * jnp.repeat(heights, shape[axis_at] // parts).reshape([-1 if axis == axis_at else 1 for axis in range(len(shape))])
    return level


def gaussian(rng, extent, scale, reach, cuts=(), kind=jnp.bfloat16):
    entries = jax.random.normal(rng, extent, jnp.float32) * scale
    if len(cuts) > 0:
        entries = block_levels(rng, extent, cuts, -0.22, 0.18) * entries
    return jnp.clip(entries, min=-reach, max=reach).astype(kind)


def setup_inputs(seed: int = 0) -> dict:
    key_list = jax.random.split(jax.random.key(seed), 8)
    return {
        "hamiltonian": gaussian(key_list[0], (NB, M, M), M ** -0.5, 0.5, ((0, 8),), jnp.float32),
        "coupling": gaussian(key_list[1], (NB, INTERFACE, INTERFACE), INTERFACE ** -0.5, 0.75, ((0, 8),), jnp.float32),
        "contact_rates": jnp.clip(jnp.exp(jax.random.uniform(key_list[2], (2, INTERFACE), jnp.float32, math.log(0.2), math.log(2.0))), 0.2, 2.0),
        "occupation": jnp.clip(1.0 * jax.random.uniform(key_list[3], (E_DEV, N_ENERGY, 2), jnp.float32) ** block_levels(key_list[3], (E_DEV, N_ENERGY, 2), ((1, 64),), -0.2, 0.2), 0.0, 1.0),
        "lesser_in": draw_lesser_in(jax.random.fold_in(key_list[7], 71), 0),
        "greater_in": draw_greater_in(jax.random.fold_in(key_list[7], 71), 0),
        "phonon_shift": jax.random.randint(key_list[6], (1,), 1, KMAX).astype(jnp.int32),
    }


highest = lax.Precision.HIGHEST
broadening = 0.2
phonon_bose = 0.4
phonon_strength = 0.5

def matmul_high(first_factor, second_factor):
    return jnp.matmul(first_factor, second_factor, precision=highest)

def transposed(matrix):
    return jnp.swapaxes(matrix, -1, -2)

def complex_product(first_pair, second_pair):
    return (matmul_high(first_pair[0], second_pair[0]) - matmul_high(first_pair[1], second_pair[1]), matmul_high(first_pair[0], second_pair[1]) + matmul_high(first_pair[1], second_pair[0]))

def adjoint(complex_pair):
    return (transposed(complex_pair[0]), -transposed(complex_pair[1]))

def inverted(complex_pair):
    real_part, imag_part = complex_pair
    orbitals = real_part.shape[-1]
    stacked = jnp.concatenate([jnp.concatenate([real_part, -imag_part], -1), jnp.concatenate([imag_part, real_part], -1)], -2)
    target = jnp.concatenate([jnp.eye(orbitals, dtype=jnp.float32), jnp.zeros((orbitals, orbitals), jnp.float32)], 0)
    target = jnp.broadcast_to(target, stacked.shape[:-2] + target.shape)
    solved = jnp.linalg.solve(stacked, target)
    return (solved[..., :orbitals, :], solved[..., orbitals:, :])

def pad_first(corner, orbitals):
    extra = orbitals - corner.shape[-1]
    return jnp.pad(corner, ((0, 0), (0, extra), (0, extra)))

def pad_last(corner, orbitals):
    extra = orbitals - corner.shape[-1]
    return jnp.pad(corner, ((0, 0), (extra, 0), (extra, 0)))

def reference(hamiltonian, coupling, contact_rates, occupation, lesser_in, greater_in, phonon_shift):
    blocks = hamiltonian.shape[0]
    orbitals = hamiltonian.shape[1]
    interface = coupling.shape[1]
    energies = lesser_in.shape[0] * lesser_in.shape[1]
    lesser_all = jnp.swapaxes(lesser_in.reshape((energies,) + lesser_in.shape[2:]), 0, 1)
    greater_all = jnp.swapaxes(greater_in.reshape((energies,) + greater_in.shape[2:]), 0, 1)
    filling = occupation.reshape(energies, 2)
    energy_index = jnp.arange(energies, dtype=jnp.int32)
    energy_value = -1.5 + 3.0 * energy_index.astype(jnp.float32) / (energies - 1)
    identity = jnp.eye(orbitals, dtype=jnp.float32)
    extra = orbitals - interface
    gamma_left = jnp.pad(jnp.diag(contact_rates[0]), ((0, extra), (0, extra)))
    last_coupling = coupling[blocks - 1]
    gamma_right = jnp.pad(matmul_high(last_coupling * contact_rates[1][None, :], transposed(last_coupling)), ((extra, 0), (extra, 0)))
    block_index = jnp.arange(blocks, dtype=jnp.int32)
    first_flags = (block_index == 0).astype(jnp.float32)
    last_flags = (block_index == blocks - 1).astype(jnp.float32)

    def system(hamiltonian_block, lesser_block, greater_block, first_flag, last_flag):
        onsite = 0.5 * (hamiltonian_block + hamiltonian_block.T)
        matrix_real = energy_value[:, None, None] * identity - onsite - 0.5 * (greater_block[:, 0] - lesser_block[:, 0])
        matrix_imag = broadening * identity - 0.5 * (greater_block[:, 1] - lesser_block[:, 1])
        matrix_imag = matrix_imag + 0.5 * first_flag * gamma_left
        matrix_imag = matrix_imag + 0.5 * last_flag * gamma_right
        source_imag = lesser_block[:, 1] + first_flag * filling[:, 0, None, None] * gamma_left
        source_imag = source_imag + last_flag * filling[:, 1, None, None] * gamma_right
        return ((matrix_real, matrix_imag), (lesser_block[:, 0], source_imag))

    def forward(boundary, inputs):
        hamiltonian_block, link_block, lesser_block, greater_block, first_flag, last_flag = inputs
        matrix, source = system(hamiltonian_block, lesser_block, greater_block, first_flag, last_flag)
        matrix = (matrix[0] - pad_first(boundary[0], orbitals), matrix[1] - pad_first(boundary[1], orbitals))
        source = (source[0] + pad_first(boundary[2], orbitals), source[1] + pad_first(boundary[3], orbitals))
        green_block = inverted(matrix)
        lesser_green = complex_product(complex_product(green_block, source), adjoint(green_block))
        corners = jnp.stack([green_block[0][..., -interface:, -interface:], green_block[1][..., -interface:, -interface:], lesser_green[0][..., -interface:, -interface:], lesser_green[1][..., -interface:, -interface:]])
        next_boundary = matmul_high(transposed(link_block), matmul_high(corners, link_block))
        return (next_boundary, jnp.stack([green_block[0], green_block[1], lesser_green[0], lesser_green[1]]))
    start = jnp.zeros((4, energies, interface, interface), jnp.float32)
    _, forward_store = lax.scan(forward, start, (hamiltonian, coupling, lesser_all, greater_all, first_flags, last_flags))

    def backward(corner, inputs):
        saved, link_block = inputs
        green_block = (saved[0], saved[1])
        lesser_block = (saved[2], saved[3])
        coupled_all = matmul_high(link_block, matmul_high(corner, transposed(link_block)))
        coupled = (coupled_all[0], coupled_all[1])
        coupled_lesser = (coupled_all[2], coupled_all[3])
        column = (green_block[0][..., -interface:], green_block[1][..., -interface:])
        green_row = (green_block[0][..., -interface:, :], green_block[1][..., -interface:, :])
        lesser_column = (lesser_block[0][..., -interface:], lesser_block[1][..., -interface:])
        lesser_row = (lesser_block[0][..., -interface:, :], lesser_block[1][..., -interface:, :])
        weighted = complex_product(column, coupled)
        column_adjoint = adjoint(column)
        update = complex_product(weighted, green_row)
        full_green = (green_block[0] + update[0], green_block[1] + update[1])
        first_term = complex_product(complex_product(column, coupled_lesser), column_adjoint)
        second_term = complex_product(weighted, lesser_row)
        third_term = complex_product(lesser_column, complex_product(adjoint(coupled), column_adjoint))
        full_lesser = (lesser_block[0] + first_term[0] + second_term[0] + third_term[0], lesser_block[1] + first_term[1] + second_term[1] + third_term[1])
        new_corner = jnp.stack([full_green[0][..., :interface, :interface], full_green[1][..., :interface, :interface], full_lesser[0][..., :interface, :interface], full_lesser[1][..., :interface, :interface]])
        return (new_corner, jnp.stack([full_green[0], full_green[1], full_lesser[0], full_lesser[1]]))
    _, final_store = lax.scan(backward, start, (forward_store, coupling), reverse=True)
    green_real = final_store[:, 0]
    green_imag = final_store[:, 1]
    lesser_real = final_store[:, 2]
    lesser_imag = final_store[:, 3]
    greater_real = lesser_real + green_real - transposed(green_real)
    greater_imag = lesser_imag + green_imag + transposed(green_imag)
    amount = phonon_shift[0]

    def shifted(field, offset):
        rolled = jnp.roll(field, offset, axis=1)
        source_index = energy_index - offset
        valid_mask = ((source_index >= 0) & (source_index < energies)).astype(jnp.float32)
        return rolled * valid_mask[None, :, None, None]
    lesser_out_real = phonon_strength * ((phonon_bose + 1.0) * shifted(lesser_real, -amount) + phonon_bose * shifted(lesser_real, amount))
    lesser_out_imag = phonon_strength * ((phonon_bose + 1.0) * shifted(lesser_imag, -amount) + phonon_bose * shifted(lesser_imag, amount))
    greater_out_real = phonon_strength * ((phonon_bose + 1.0) * shifted(greater_real, amount) + phonon_bose * shifted(greater_real, -amount))
    greater_out_imag = phonon_strength * ((phonon_bose + 1.0) * shifted(greater_imag, amount) + phonon_bose * shifted(greater_imag, -amount))
    lesser_out = jnp.swapaxes(jnp.stack([lesser_out_real, lesser_out_imag], 2), 0, 1).reshape(lesser_in.shape)
    greater_out = jnp.swapaxes(jnp.stack([greater_out_real, greater_out_imag], 2), 0, 1).reshape(greater_in.shape)
    return (lesser_out, greater_out)
```

```python
import functools

import jax
import jax.numpy as jnp
from jax import lax
from jax.experimental import pallas as pl
from jax.experimental.pallas import tpu as pltpu
from jax.sharding import PartitionSpec as P

HALF = 64
FULL = 128
broadening = 0.2
phonon_bose = 0.4
phonon_strength = 0.5
quantum_bound = 32
highest = lax.Precision.HIGHEST


def iota(shape, axis):
    return lax.broadcasted_iota(jnp.int32, shape, axis)


def dot(a, b):
    return lax.dot_general(
        a, b, (((1,), (0,)), ((), ())), precision=highest, preferred_element_type=jnp.float32
    )


def dot_nt(a, b):
    return lax.dot_general(
        a, b, (((1,), (1,)), ((), ())), precision=highest, preferred_element_type=jnp.float32
    )


def rolled(x):
    return jnp.concatenate([x[:, HALF:], x[:, :HALF]], axis=1)


def blocks(x):
    return [x[:, at:at + FULL] for at in range(0, x.shape[1], FULL)]


def lanes(parts):
    return parts[0] if len(parts) == 1 else jnp.concatenate(parts, axis=1)


def rows(parts):
    return parts[0] if len(parts) == 1 else jnp.concatenate(parts, axis=0)


def times_i(x):
    parts = []
    for block in blocks(x):
        turned = rolled(block)
        parts.append(jnp.where(iota(block.shape, 1) < HALF, -turned, turned))
    return lanes(parts)


def expanded(x):
    twin = times_i(x)
    parts = []
    for at in range(0, x.shape[0], HALF):
        parts += [x[at:at + HALF], twin[at:at + HALF]]
    return rows(parts)


def product(a, b):
    return dot(a, expanded(b))


def product_adjoint(a, b):
    return dot_nt(a, expanded(b))


def unit():
    shape = (HALF, FULL)
    return jnp.where(iota(shape, 0) == iota(shape, 1), 1.0, 0.0)


def spread(x, lane):
    return jnp.broadcast_to(x[:, lane:lane + 1], (x.shape[0], FULL))


def inverse(a):
    row4 = iota((4, FULL), 0)
    lane4 = iota((4, FULL), 1)
    wide = iota((HALF, FULL), 1) & (HALF - 1)
    for k in range(0, HALF, 4):
        col_re = [spread(a, k + j) for j in range(4)]
        col_im = [spread(a, HALF + k + j) for j in range(4)]
        local = lane4 & (HALF - 1)
        here = (local >= k) & (local < k + 4)
        ones = jnp.where(lane4 == row4 + k, 1.0, 0.0)
        panel = jnp.where(here, ones, a[k:k + 4])
        twin = times_i(panel)
        piv_re = [c[k:k + 4] for c in col_re]
        piv_im = [c[k:k + 4] for c in col_im]
        for j in range(4):
            p_re, p_im = piv_re[j][j:j + 1], piv_im[j][j:j + 1]
            scale = 1.0 / (p_re * p_re + p_im * p_im)
            q_re, q_im = p_re * scale, -(p_im * scale)
            r, t = panel[j:j + 1], twin[j:j + 1]
            new_r = q_re * r + q_im * t
            new_t = q_re * t - q_im * r
            f_re, f_im = piv_re[j], piv_im[j]
            mine = row4 == j
            panel = jnp.where(mine, new_r, panel - (f_re * new_r + f_im * new_t))
            twin = jnp.where(mine, new_t, twin - (f_re * new_t - f_im * new_r))
            for l in range(j + 1, 4):
                u, v = piv_re[l][j:j + 1], piv_im[l][j:j + 1]
                s_re = q_re * u - q_im * v
                s_im = q_re * v + q_im * u
                piv_re[l] = jnp.where(mine, s_re, piv_re[l] - (f_re * s_re - f_im * s_im))
                piv_im[l] = jnp.where(mine, s_im, piv_im[l] - (f_re * s_im + f_im * s_re))
        rest = jnp.where((wide >= k) & (wide < k + 4), 0.0, a)
        for j in range(4):
            rest = rest - (col_re[j] * panel[j:j + 1] + col_im[j] * twin[j:j + 1])
        a = rows([p for p in (rest[:k], panel, rest[k + 4:]) if p.shape[0]])
    return a


def inverse_full(a):
    left, right = blocks(a)
    first = inverse(left[:HALF])
    below = product(left[HALF:], first)
    last = inverse(right[HALF:] - product(below, right[:HALF]))
    ahead = product(first, right[:HALF])
    edges = product(rows([ahead]), last)
    low = -product(last, below)
    top = first + product(edges, below)
    return lanes([rows([top, low]), rows([-edges, last])])


def resolved(sigma_g):
    return inverse(unit() - sigma_g)


def updated(phi, f, sigma, v_extra, k_in, kh_in, k_nn, kh_nn, g_row, gh_row, k_row, kh_row, g0, k0):
    count = f.shape[0]
    u = product(f, phi)
    v = product(u, sigma)
    if v_extra is not None:
        v = rows([v[:FULL], v[FULL:] + v_extra])
    l_own = k_in + product(v, k_nn)
    l_other = product(u, kh_nn)
    if kh_in is not None:
        l_other = rows([l_other[:FULL], l_other[FULL:] + kh_in])
    both = lanes([v, u])
    spread_rows = rows([
        rows([both[at:at + HALF], times_i(both[at:at + HALF])]) for at in range(0, count, HALF)
    ])
    if gh_row is None:
        right = expanded(lanes([g_row, k_row]))
        grown = dot(v, right)
    else:
        own = expanded(lanes([g_row, k_row]))
        other = expanded(lanes([gh_row, kh_row]))
        grown = dot(both, rows([own, other]))
    width = g0.shape[1]
    g = g0 + grown[:, :width]
    k = k0 + grown[:, width:] + dot_nt(lanes([l_own, l_other]), spread_rows)
    return g, k


def packed_columns(re, im):
    first = iota(re.shape, 1) < HALF
    return lanes([jnp.where(first, re, rolled(im)), jnp.where(first, rolled(re), im)])


def planes(x):
    left, right = blocks(x)
    first = iota(left.shape, 1) < HALF
    return jnp.where(first, left, rolled(right)), jnp.where(first, rolled(left), right)


def flipped(flag, x):
    turned = rows([x[HALF:], x[:HALF]])
    left, right = blocks(turned)
    return jnp.where(flag, lanes([right, left]), x)


def isolated_kernel(h_ref, c_ref, rates_ref, occ_ref, lesser_ref, greater_ref, g_ref, k_ref):
    dom = lax.axis_index("dom")
    energy = lax.axis_index("energy")
    energies = lax.axis_size("energy")
    odd = dom % 2 == 1
    at_left = jnp.where(dom == 0, 1.0, 0.0)
    at_right = jnp.where(dom == lax.axis_size("dom") - 1, 1.0, 0.0)
    shape = (FULL, FULL)
    h = h_ref[0]
    lesser_re, lesser_im = lesser_ref[0, 0, 0, 0], lesser_ref[0, 0, 0, 1]
    greater_re, greater_im = greater_ref[0, 0, 0, 0], greater_ref[0, 0, 0, 1]
    diagonal = iota(shape, 0) == iota(shape, 1)
    index = jnp.full(shape, energy, jnp.int32).astype(jnp.float32)
    value = -1.5 + 3.0 * index / (energies - 1)
    left_rates = lanes([rates_ref[0:1], jnp.zeros((1, HALF), jnp.float32)])
    gamma_left = jnp.where(diagonal, left_rates, 0.0)
    c = c_ref[0]
    corner = dot_nt(c * rates_ref[1:2], c)
    zero = jnp.zeros((HALF, HALF), jnp.float32)
    gamma_right = rows([jnp.zeros((HALF, FULL), jnp.float32), lanes([zero, corner])])
    re = jnp.where(diagonal, value, 0.0) - 0.5 * (h + h.T) - 0.5 * (greater_re - lesser_re)
    im = jnp.where(diagonal, broadening, 0.0) - 0.5 * (greater_im - lesser_im)
    im = im + (0.5 * at_left) * gamma_left + (0.5 * at_right) * gamma_right
    source_im = (
        lesser_im
        + (at_left * occ_ref[0, 0, 0]) * gamma_left
        + (at_right * occ_ref[0, 0, 1]) * gamma_right
    )
    g = inverse_full(flipped(odd, packed_columns(re, im)))
    source = flipped(odd, packed_columns(lesser_re, source_im))
    g_ref[...] = g
    k_ref[...] = product_adjoint(product(g, source), g)


def pair_kernel(c_ref, c_other_ref, c_before_ref, c_before2_ref, g_ref, k_ref, gp_ref, kp_ref,
                g_out, k_out, mg_out, mk_out):
    dom = lax.axis_index("dom")
    odd = dom % 2 == 1
    side = (dom // 2) % 2
    c, c_other = c_ref[0], c_other_ref[0]
    tau = jnp.where(odd, c_other.T, c)
    g, k, gp, kp = g_ref[...], k_ref[...], gp_ref[...], kp_ref[...]
    (gf, gn), (kf, kn) = blocks(g), blocks(k)
    (gpf, gpn), (kpf, kpn) = blocks(gp), blocks(kp)
    tall = dot(tau, lanes([gpn[HALF:], kpn[HALF:], gpf[HALF:], kpf[HALF:]]))
    nn_g, nn_k, gh_nf, kh_nf = blocks(tall)
    sides = dot_nt(rows([nn_g, nn_k, gpn[:HALF], kpn[:HALF]]), real_pair(tau))
    sigma, sigma_k, gh_fn, kh_fn = (sides[at:at + HALF] for at in range(0, 4 * HALF, HALF))
    g_nn, k_nn = gn[HALF:], kn[HALF:]
    mixed = product(rows([sigma, gh_fn]), g_nn)
    phi = resolved(mixed[:HALF])
    f = rows([gn, mixed[HALF:]])
    zero = jnp.zeros((HALF, FULL), jnp.float32)
    zero2 = lanes([zero, zero])
    k_in = rows([kn, zero])
    g0 = rows([lanes([g, jnp.zeros((FULL, FULL), jnp.float32)]), lanes([zero2, gpf[:HALF]])])
    k0 = rows([lanes([k, jnp.zeros((FULL, FULL), jnp.float32)]), lanes([zero2, kpf[:HALF]])])
    g1, k1 = updated(
        phi, f, sigma, gh_fn, k_in, kh_fn, k_nn, sigma_k,
        lanes([g[HALF:], zero]), lanes([zero2, gh_nf]),
        lanes([k[HALF:], zero]), lanes([zero2, kh_nf]), g0, k0,
    )
    g_out[...] = g1
    k_out[...] = k1
    last = jnp.where(odd, c, c_other)
    before = jnp.where(odd, c_before2_ref[0], c_before_ref[0])
    kappa = jnp.where(side == 1, before, last.T)
    for x, out in ((g1, mg_out), (k1, mk_out)):
        b0, _, b2 = blocks(x)
        ports = rows([lanes([b0[:HALF], b2[:HALF]]), lanes([b0[FULL:], b2[FULL:]])])
        ports = flipped(odd != (side == 1), ports)
        pf, pn = blocks(ports)
        tall = dot(kappa, ports[HALF:])
        wide = dot_nt(rows([pn[:HALF], tall[:, FULL:]]), real_pair(kappa))
        out[...] = lanes([rows([pf[:HALF], tall[:, :FULL]]), wide])


def real_pair(tau):
    zero = jnp.zeros_like(tau)
    return rows([lanes([tau, zero]), lanes([zero, tau])])


def quad_kernel(c_ref, c_other_ref, c_before_ref, c_before2_ref, g_ref, k_ref, gp_ref, kp_ref,
                g_out, k_out, mg_out, mk_out):
    dom = lax.axis_index("dom")
    odd = dom % 2 == 1
    place = dom // 2
    side = place % 2
    edge = (place == 0) | (place == 3)
    outer = odd == (side == 1)
    g, k, gp, kp = g_ref[...], k_ref[...], gp_ref[...], kp_ref[...]

    def near_far_columns(x):
        b0, _, b2 = blocks(x)
        return jnp.where(outer, b2, b0), jnp.where(outer, b0, b2)

    def near_far_rows(x):
        return jnp.where(outer, x[FULL:], x[:HALF]), jnp.where(outer, x[:HALF], x[FULL:])

    gc_n, gc_f = near_far_columns(g)
    kc_n, kc_f = near_far_columns(k)
    gr_n, gr_f = near_far_rows(g)
    kr_n, kr_f = near_far_rows(k)
    g_nn, g_fn = near_far_rows(gc_n)
    k_nn, k_fn = near_far_rows(kc_n)
    g_nf, g_ff = near_far_rows(gc_f)
    k_nf, k_ff = near_far_rows(kc_f)
    gpf, gpn = blocks(gp)
    kpf, kpn = blocks(kp)
    sigma, sigma_k = gpn[HALF:], kpn[HALF:]
    gh_fn, kh_fn = gpn[:HALF], kpn[:HALF]
    mixed = product(gpn, g_nn)
    phi = resolved(mixed[HALF:])
    zero = jnp.zeros((HALF, FULL), jnp.float32)
    f = rows([gc_n[:FULL], jnp.where(edge, mixed[:HALF], g_fn)])
    k_in = rows([kc_n[:FULL], jnp.where(edge, 0.0, k_fn)])
    zero2 = lanes([zero, zero])

    def row(own, own_q, other_q):
        return lanes([own, jnp.where(edge, 0.0, own_q)]), lanes([zero2, jnp.where(edge, other_q, 0.0)])

    g_row, gh_row = row(gr_n[:, :2 * FULL], g_nf, gpf[HALF:])
    k_row, kh_row = row(kr_n[:, :2 * FULL], k_nf, kpf[HALF:])

    def base(x, x_mf, x_fm, x_ff, other_ff):
        top = lanes([x[:FULL, :2 * FULL], jnp.where(edge, 0.0, x_mf)])
        low = lanes([jnp.where(edge, 0.0, x_fm), jnp.where(edge, other_ff, x_ff)])
        return rows([top, low])

    g2, k2 = updated(
        phi, f, sigma, jnp.where(edge, gh_fn, 0.0), k_in, jnp.where(edge, kh_fn, 0.0), k_nn, sigma_k,
        g_row, gh_row, k_row, kh_row,
        base(g, gc_f[:FULL], gr_f[:, :2 * FULL], g_ff, gpf[:HALF]),
        base(k, kc_f[:FULL], kr_f[:, :2 * FULL], k_ff, kpf[:HALF]),
    )
    g_out[...] = g2
    k_out[...] = k2
    last = jnp.where(odd, c_ref[0], c_other_ref[0])
    before = jnp.where(odd, c_before2_ref[0], c_before_ref[0])
    kappa = jnp.where(place == 1, last.T, before)
    tall = dot(kappa, lanes([g2[FULL:, 2 * FULL:], k2[FULL:, 2 * FULL:]]))
    wide = dot_nt(rows(blocks(tall)), real_pair(kappa))
    mg_out[...] = wide[:HALF]
    mk_out[...] = wide[HALF:]


def final_kernel(g_ref, k_ref, ga_ref, gb_ref, ka_ref, kb_ref, out_ref):
    odd = lax.axis_index("dom") % 2 == 1
    g, k = g_ref[...], k_ref[...]
    sigma = ga_ref[...] + gb_ref[...]
    sigma_k = ka_ref[...] + kb_ref[...]
    g_mn, k_mn = g[:FULL, 2 * FULL:], k[:FULL, 2 * FULL:]
    g_nn, k_nn = g[FULL:, 2 * FULL:], k[FULL:, 2 * FULL:]
    phi = resolved(product(sigma, g_nn))
    g3, k3 = updated(
        phi, g_mn, sigma, None, k_mn, None, k_nn, sigma_k,
        g[FULL:, :2 * FULL], None, k[FULL:, :2 * FULL], None,
        g[:FULL, :2 * FULL], k[:FULL, :2 * FULL],
    )
    g_re, g_im = planes(flipped(odd, g3))
    k_re, k_im = planes(flipped(odd, k3))
    lower = iota((FULL, FULL), 0) > iota((FULL, FULL), 1)
    out_ref[0] = jnp.where(lower, k_re, k_im)
    out_ref[1] = jnp.where(lower, k_re + g_re - g_re.T, k_im + g_im + g_im.T)


def scatter_kernel(above_ref, below_ref, lesser_ref, greater_ref):
    shape = (FULL, FULL)
    lower = iota(shape, 0) > iota(shape, 1)
    upper = iota(shape, 0) < iota(shape, 1)
    strong = phonon_strength * (phonon_bose + 1.0)
    weak = phonon_strength * phonon_bose
    mixes = (
        strong * above_ref[0] + weak * below_ref[0],
        strong * below_ref[1] + weak * above_ref[1],
    )
    for mix, out in zip(mixes, (lesser_ref, greater_ref)):
        flip = mix.T
        out[0, 0, 0, 0] = jnp.where(lower, mix, jnp.where(upper, -flip, 0.0))
        out[0, 0, 0, 1] = jnp.where(lower, flip, mix)


def call(kernel, shapes, *operands, scalars=()):
    specs = [
        pl.BlockSpec(memory_space=pltpu.SMEM if at in scalars else pltpu.VMEM)
        for at in range(len(operands))
    ]
    out = [jax.ShapeDtypeStruct(shape, jnp.float32) for shape in shapes]
    return pl.pallas_call(
        kernel,
        out_shape=out,
        in_specs=specs,
        out_specs=[pl.BlockSpec(memory_space=pltpu.VMEM)] * len(out),
        compiler_params=pltpu.CompilerParams(vmem_limit_bytes=48 * 2**20),
        cost_estimate=pl.CostEstimate(flops=10**9, bytes_accessed=10**6, transcendentals=0),
    )(*operands)


def permuted(value, pairs):
    return lax.ppermute(value, "dom", pairs)


def on_device(
    hamiltonian, coupling, contact_rates, occupation, lesser_in, greater_in, phonon_shift
):
    count = lax.axis_size("energy")
    swap1 = [(b, b ^ 1) for b in range(8)]
    swap2 = [(b, b ^ 2) for b in range(8)]
    inner = [(2, 4), (3, 5), (4, 2), (5, 3)]
    outer = [(2, 6), (3, 7), (4, 0), (5, 1)]
    c_other = permuted(coupling, swap1)
    c_before = permuted(coupling, [(b, b + 1) for b in (1, 3, 5)])
    c_before2 = permuted(coupling, [(b, b + 2) for b in (1, 3, 5)])
    couplings = (coupling, c_other, c_before, c_before2)
    port2 = (FULL, 2 * FULL)
    state = (FULL + HALF, 3 * FULL)
    port1 = (HALF, FULL)
    g, k = call(
        isolated_kernel, [port2, port2], hamiltonian, coupling, contact_rates, occupation,
        lesser_in, greater_in, scalars=(3,),
    )
    gp, kp = permuted(g, swap1), permuted(k, swap1)
    g, k, mg, mk = call(
        pair_kernel, [state, state, port2, port2], *couplings, g, k, gp, kp
    )
    gp, kp = permuted(mg, swap2), permuted(mk, swap2)
    g, k, mg, mk = call(
        quad_kernel, [state, state, port1, port1], *couplings, g, k, gp, kp
    )
    payload = call(
        final_kernel, [(2, FULL, FULL)], g, k,
        permuted(mg, inner), permuted(mg, outer), permuted(mk, inner), permuted(mk, outer),
    )[0]

    def shifted(steps):
        def branch(value):
            ups = [(e, e + steps) for e in range(count - steps)]
            downs = [(e + steps, e) for e in range(count - steps)]
            return lax.ppermute(value, "energy", downs), lax.ppermute(value, "energy", ups)

        return branch

    amount = jnp.clip(phonon_shift[0], 0, min(quantum_bound, count) - 1)
    above, below = lax.switch(
        amount, [shifted(steps) for steps in range(min(quantum_bound, count))], payload
    )
    out = (1, 1, 1, 2, FULL, FULL)
    return tuple(call(scatter_kernel, [out, out], above, below))


def solution(mesh):
    blocks_spec = P(None, "energy", "dom", None, None, None)
    return jax.shard_map(
        on_device,
        mesh=mesh,
        in_specs=(
            P("dom", None, None),
            P("dom", None, None),
            P(),
            P(None, "energy", None),
            blocks_spec,
            blocks_spec,
            P(),
        ),
        out_specs=(blocks_spec, blocks_spec),
        check_vma=False,
    )
```

```python
import functools

import jax
import jax.numpy as jnp
from jax import lax
from jax.experimental import pallas as pl
from jax.experimental.pallas import tpu as pltpu
from jax.sharding import PartitionSpec as P

HALF = 64
FULL = 128
broadening = 0.2
phonon_bose = 0.4
phonon_strength = 0.5
quantum_bound = 32
fine = 4


def iota(shape, axis):
    return lax.broadcasted_iota(jnp.int32, shape, axis)


def halves(x):
    high = x.astype(jnp.bfloat16)
    return high, (x - high.astype(jnp.float32)).astype(jnp.bfloat16)


def three_passes(a, b, contracted):
    count = a.shape[0]
    (a_high, a_low), (b_high, b_low) = halves(a), halves(b)
    dims = (((1,), (contracted,)), ((), ()))
    main = lax.dot_general(rows([a_high, a_low]), b_high, dims, preferred_element_type=jnp.float32)
    rest = lax.dot_general(a_high, b_low, dims, preferred_element_type=jnp.float32)
    return main[:count] + (main[count:] + rest)


def dot(a, b):
    return three_passes(a, b, 0)


def dot_nt(a, b):
    return three_passes(a, b, 1)


def rolled(x):
    return jnp.concatenate([x[:, HALF:], x[:, :HALF]], axis=1)


def blocks(x):
    return [x[:, at:at + FULL] for at in range(0, x.shape[1], FULL)]


def lanes(parts):
    return parts[0] if len(parts) == 1 else jnp.concatenate(parts, axis=1)


def rows(parts):
    return parts[0] if len(parts) == 1 else jnp.concatenate(parts, axis=0)


def times_i(x):
    parts = []
    for block in blocks(x):
        turned = rolled(block)
        parts.append(jnp.where(iota(block.shape, 1) < HALF, -turned, turned))
    return lanes(parts)


def expanded(x):
    twin = times_i(x)
    parts = []
    for at in range(0, x.shape[0], HALF):
        parts += [x[at:at + HALF], twin[at:at + HALF]]
    return rows(parts)


def product(a, b):
    return dot(a, expanded(b))


def product_adjoint(a, b):
    return dot_nt(a, expanded(b))


def unit():
    shape = (HALF, FULL)
    return jnp.where(iota(shape, 0) == iota(shape, 1), 1.0, 0.0)


def spread(x, lane):
    return jnp.broadcast_to(x[:, lane:lane + 1], (x.shape[0], FULL))


def inverse(a):
    row4 = iota((4, FULL), 0)
    lane4 = iota((4, FULL), 1)
    wide = iota((HALF, FULL), 1) & (HALF - 1)
    for k in range(0, HALF, 4):
        col_re = [spread(a, k + j) for j in range(4)]
        col_im = [spread(a, HALF + k + j) for j in range(4)]
        local = lane4 & (HALF - 1)
        here = (local >= k) & (local < k + 4)
        ones = jnp.where(lane4 == row4 + k, 1.0, 0.0)
        panel = jnp.where(here, ones, a[k:k + 4])
        twin = times_i(panel)
        piv_re = [c[k:k + 4] for c in col_re]
        piv_im = [c[k:k + 4] for c in col_im]
        for j in range(4):
            p_re, p_im = piv_re[j][j:j + 1], piv_im[j][j:j + 1]
            scale = 1.0 / (p_re * p_re + p_im * p_im)
            q_re, q_im = p_re * scale, -(p_im * scale)
            r, t = panel[j:j + 1], twin[j:j + 1]
            new_r = q_re * r + q_im * t
            new_t = q_re * t - q_im * r
            f_re, f_im = piv_re[j], piv_im[j]
            mine = row4 == j
            panel = jnp.where(mine, new_r, panel - (f_re * new_r + f_im * new_t))
            twin = jnp.where(mine, new_t, twin - (f_re * new_t - f_im * new_r))
            for l in range(j + 1, 4):
                u, v = piv_re[l][j:j + 1], piv_im[l][j:j + 1]
                s_re = q_re * u - q_im * v
                s_im = q_re * v + q_im * u
                piv_re[l] = jnp.where(mine, s_re, piv_re[l] - (f_re * s_re - f_im * s_im))
                piv_im[l] = jnp.where(mine, s_im, piv_im[l] - (f_re * s_im + f_im * s_re))
        rest = jnp.where((wide >= k) & (wide < k + 4), 0.0, a)
        for j in range(4):
            rest = rest - (col_re[j] * panel[j:j + 1] + col_im[j] * twin[j:j + 1])
        a = rows([p for p in (rest[:k], panel, rest[k + 4:]) if p.shape[0]])
    return a


def inverse_full(a):
    left, right = blocks(a)
    first = inverse(left[:HALF])
    below = product(left[HALF:], first)
    last = inverse(right[HALF:] - product(below, right[:HALF]))
    ahead = product(first, right[:HALF])
    edges = product(rows([ahead]), last)
    low = -product(last, below)
    top = first + product(edges, below)
    return lanes([rows([top, low]), rows([-edges, last])])


def resolved(sigma_g):
    return inverse(unit() - sigma_g)


def updated(phi, f, sigma, v_extra, k_in, kh_in, k_nn, kh_nn, g_row, gh_row, k_row, kh_row, g0, k0):
    count = f.shape[0]
    u = product(f, phi)
    v = product(u, sigma)
    if v_extra is not None:
        v = rows([v[:FULL], v[FULL:] + v_extra])
    l_own = k_in + product(v, k_nn)
    l_other = product(u, kh_nn)
    if kh_in is not None:
        l_other = rows([l_other[:FULL], l_other[FULL:] + kh_in])
    both = lanes([v, u])
    spread_rows = rows([
        rows([both[at:at + HALF], times_i(both[at:at + HALF])]) for at in range(0, count, HALF)
    ])
    if gh_row is None:
        right = expanded(lanes([g_row, k_row]))
        grown = dot(v, right)
    else:
        own = expanded(lanes([g_row, k_row]))
        other = expanded(lanes([gh_row, kh_row]))
        grown = dot(both, rows([own, other]))
    width = g0.shape[1]
    g = g0 + grown[:, :width]
    k = k0 + grown[:, width:] + dot_nt(lanes([l_own, l_other]), spread_rows)
    return g, k


def packed_columns(re, im):
    first = iota(re.shape, 1) < HALF
    return lanes([jnp.where(first, re, rolled(im)), jnp.where(first, rolled(re), im)])


def planes(x):
    left, right = blocks(x)
    first = iota(left.shape, 1) < HALF
    return jnp.where(first, left, rolled(right)), jnp.where(first, rolled(left), right)


def flipped(flag, x):
    turned = rows([x[HALF:], x[:HALF]])
    left, right = blocks(turned)
    return jnp.where(flag, lanes([right, left]), x)


def isolated_kernel(h_hbm, c_hbm, rates_hbm, occ_ref, lesser_hbm, greater_hbm, out_ref,
                    h_ref, c_ref, rates_ref, lesser_ref, greater_ref, sems):
    moves = [
        pltpu.make_async_copy(source, target, sems.at[at])
        for at, (source, target) in enumerate((
            (lesser_hbm, lesser_ref), (greater_hbm, greater_ref), (h_hbm, h_ref),
            (c_hbm, c_ref), (rates_hbm, rates_ref),
        ))
    ]
    for move in moves:
        move.start()
    for move in moves:
        move.wait()
    isolated(h_ref, c_ref, rates_ref, occ_ref, lesser_ref, greater_ref, out_ref)


def isolated(h_ref, c_ref, rates_ref, occ_ref, lesser_ref, greater_ref, out_ref):
    dom = lax.axis_index("dom")
    energy = lax.axis_index("energy")
    energies = lax.axis_size("energy")
    odd = dom % 2 == 1
    at_left = jnp.where(dom == 0, 1.0, 0.0)
    at_right = jnp.where(dom == lax.axis_size("dom") - 1, 1.0, 0.0)
    shape = (FULL, FULL)
    h = h_ref[0]
    lesser_re, lesser_im = lesser_ref[0, 0, 0, 0], lesser_ref[0, 0, 0, 1]
    greater_re, greater_im = greater_ref[0, 0, 0, 0], greater_ref[0, 0, 0, 1]
    diagonal = iota(shape, 0) == iota(shape, 1)
    index = jnp.full(shape, energy, jnp.int32).astype(jnp.float32)
    value = -1.5 + 3.0 * index / (energies - 1)
    left_rates = lanes([rates_ref[0:1], jnp.zeros((1, HALF), jnp.float32)])
    gamma_left = jnp.where(diagonal, left_rates, 0.0)
    c = c_ref[0]
    corner = dot_nt(c * rates_ref[1:2], c)
    zero = jnp.zeros((HALF, HALF), jnp.float32)
    gamma_right = rows([jnp.zeros((HALF, FULL), jnp.float32), lanes([zero, corner])])
    re = jnp.where(diagonal, value, 0.0) - 0.5 * (h + h.T) - 0.5 * (greater_re - lesser_re)
    im = jnp.where(diagonal, broadening, 0.0) - 0.5 * (greater_im - lesser_im)
    im = im + (0.5 * at_left) * gamma_left + (0.5 * at_right) * gamma_right
    source_im = (
        lesser_im
        + (at_left * occ_ref[0, 0, 0]) * gamma_left
        + (at_right * occ_ref[0, 0, 1]) * gamma_right
    )
    g = inverse_full(flipped(odd, packed_columns(re, im)))
    source = flipped(odd, packed_columns(lesser_re, source_im))
    out_ref[0] = g
    out_ref[1] = product_adjoint(product(g, source), g)


def pair_kernel(c_ref, c_other_ref, c_before_ref, c_before2_ref, own_ref, other_ref,
                g_out, k_out, message_out, middle_out):
    dom = lax.axis_index("dom")
    odd = dom % 2 == 1
    place = dom // 2
    side = place % 2
    c, c_other = c_ref[0], c_other_ref[0]
    tau = jnp.where(odd, c_other.T, c)
    g, k, gp, kp = own_ref[0], own_ref[1], other_ref[0], other_ref[1]
    (gf, gn), (kf, kn) = blocks(g), blocks(k)
    (gpf, gpn), (kpf, kpn) = blocks(gp), blocks(kp)
    tall = dot(tau, lanes([gpn[HALF:], kpn[HALF:], gpf[HALF:], kpf[HALF:]]))
    nn_g, nn_k, gh_nf, kh_nf = blocks(tall)
    sides = dot_nt(rows([nn_g, nn_k, gpn[:HALF], kpn[:HALF]]), real_pair(tau))
    sigma, sigma_k, gh_fn, kh_fn = (sides[at:at + HALF] for at in range(0, 4 * HALF, HALF))
    g_nn, k_nn = gn[HALF:], kn[HALF:]
    mixed = product(rows([sigma, gh_fn]), g_nn)
    phi = resolved(mixed[:HALF])
    f = rows([gn, mixed[HALF:]])
    zero = jnp.zeros((HALF, FULL), jnp.float32)
    zero2 = lanes([zero, zero])
    k_in = rows([kn, zero])
    g0 = rows([lanes([g, jnp.zeros((FULL, FULL), jnp.float32)]), lanes([zero2, gpf[:HALF]])])
    k0 = rows([lanes([k, jnp.zeros((FULL, FULL), jnp.float32)]), lanes([zero2, kpf[:HALF]])])
    g1, k1 = updated(
        phi, f, sigma, gh_fn, k_in, kh_fn, k_nn, sigma_k,
        lanes([g[HALF:], zero]), lanes([zero2, gh_nf]),
        lanes([k[HALF:], zero]), lanes([zero2, kh_nf]), g0, k0,
    )
    g_out[...] = g1
    k_out[...] = k1
    last = jnp.where(odd, c, c_other)
    before = jnp.where(odd, c_before2_ref[0], c_before_ref[0])
    kappa = jnp.where(side == 1, before, last.T)
    middle_out[0] = jnp.where(place == 1, last, before)
    for at, x in enumerate((g1, k1)):
        b0, _, b2 = blocks(x)
        ports = rows([lanes([b0[:HALF], b2[:HALF]]), lanes([b0[FULL:], b2[FULL:]])])
        ports = flipped(odd != (side == 1), ports)
        pf, pn = blocks(ports)
        tall = dot(kappa, ports[HALF:])
        wide = dot_nt(rows([pn[:HALF], tall[:, FULL:]]), real_pair(kappa))
        message_out[at] = lanes([rows([pf[:HALF], tall[:, :FULL]]), wide])


def real_pair(tau):
    zero = jnp.zeros_like(tau)
    return rows([lanes([tau, zero]), lanes([zero, tau])])


def quad_kernel(middle_own_ref, middle_other_ref, g_ref, k_ref, other_ref,
                g_out, k_out, message_out):
    dom = lax.axis_index("dom")
    odd = dom % 2 == 1
    place = dom // 2
    side = place % 2
    edge = (place == 0) | (place == 3)
    outer = odd == (side == 1)
    g, k, gp, kp = g_ref[...], k_ref[...], other_ref[0], other_ref[1]

    def near_far_columns(x):
        b0, _, b2 = blocks(x)
        return jnp.where(outer, b2, b0), jnp.where(outer, b0, b2)

    def near_far_rows(x):
        return jnp.where(outer, x[FULL:], x[:HALF]), jnp.where(outer, x[:HALF], x[FULL:])

    gc_n, gc_f = near_far_columns(g)
    kc_n, kc_f = near_far_columns(k)
    gr_n, gr_f = near_far_rows(g)
    kr_n, kr_f = near_far_rows(k)
    g_nn, g_fn = near_far_rows(gc_n)
    k_nn, k_fn = near_far_rows(kc_n)
    g_nf, g_ff = near_far_rows(gc_f)
    k_nf, k_ff = near_far_rows(kc_f)
    gpf, gpn = blocks(gp)
    kpf, kpn = blocks(kp)
    sigma, sigma_k = gpn[HALF:], kpn[HALF:]
    gh_fn, kh_fn = gpn[:HALF], kpn[:HALF]
    mixed = product(gpn, g_nn)
    phi = resolved(mixed[HALF:])
    zero = jnp.zeros((HALF, FULL), jnp.float32)
    f = rows([gc_n[:FULL], jnp.where(edge, mixed[:HALF], g_fn)])
    k_in = rows([kc_n[:FULL], jnp.where(edge, 0.0, k_fn)])
    zero2 = lanes([zero, zero])

    def row(own, own_q, other_q):
        return lanes([own, jnp.where(edge, 0.0, own_q)]), lanes([zero2, jnp.where(edge, other_q, 0.0)])

    g_row, gh_row = row(gr_n[:, :2 * FULL], g_nf, gpf[HALF:])
    k_row, kh_row = row(kr_n[:, :2 * FULL], k_nf, kpf[HALF:])

    def base(x, x_mf, x_fm, x_ff, other_ff):
        top = lanes([x[:FULL, :2 * FULL], jnp.where(edge, 0.0, x_mf)])
        low = lanes([jnp.where(edge, 0.0, x_fm), jnp.where(edge, other_ff, x_ff)])
        return rows([top, low])

    g2, k2 = updated(
        phi, f, sigma, jnp.where(edge, gh_fn, 0.0), k_in, jnp.where(edge, kh_fn, 0.0), k_nn, sigma_k,
        g_row, gh_row, k_row, kh_row,
        base(g, gc_f[:FULL], gr_f[:, :2 * FULL], g_ff, gpf[:HALF]),
        base(k, kc_f[:FULL], kr_f[:, :2 * FULL], k_ff, kpf[:HALF]),
    )
    g_out[...] = g2
    k_out[...] = k2
    middle = jnp.where(edge, middle_other_ref[0], middle_own_ref[0])
    kappa = jnp.where(place < 2, middle.T, middle)
    tall = dot(kappa, lanes([g2[FULL:, 2 * FULL:], k2[FULL:, 2 * FULL:]]))
    wide = dot_nt(rows(blocks(tall)), real_pair(kappa))
    message_out[0] = wide[:HALF]
    message_out[1] = wide[HALF:]


def final_kernel(g_ref, k_ref, other_ref, out_ref):
    odd = lax.axis_index("dom") % 2 == 1
    g, k = g_ref[...], k_ref[...]
    sigma, sigma_k = other_ref[0], other_ref[1]
    g_mn, k_mn = g[:FULL, 2 * FULL:], k[:FULL, 2 * FULL:]
    g_nn, k_nn = g[FULL:, 2 * FULL:], k[FULL:, 2 * FULL:]
    phi = resolved(product(sigma, g_nn))
    g3, k3 = updated(
        phi, g_mn, sigma, None, k_mn, None, k_nn, sigma_k,
        g[FULL:, :2 * FULL], None, k[FULL:, :2 * FULL], None,
        g[:FULL, :2 * FULL], k[:FULL, :2 * FULL],
    )
    g_re, g_im = planes(flipped(odd, g3))
    k_re, k_im = planes(flipped(odd, k3))
    lower = iota((FULL, FULL), 0) > iota((FULL, FULL), 1)
    out_ref[0] = jnp.where(lower, k_re, k_im)
    out_ref[1] = jnp.where(lower, k_re + g_re - g_re.T, k_im + g_im + g_im.T)


def scatter_kernel(above_ref, below_ref, lesser_ref, greater_ref):
    shape = (FULL, FULL)
    lower = iota(shape, 0) > iota(shape, 1)
    upper = iota(shape, 0) < iota(shape, 1)
    strong = phonon_strength * (phonon_bose + 1.0)
    weak = phonon_strength * phonon_bose
    mixes = (
        strong * above_ref[0] + weak * below_ref[0],
        strong * below_ref[1] + weak * above_ref[1],
    )
    for mix, out in zip(mixes, (lesser_ref, greater_ref)):
        flip = mix.T
        out[0, 0, 0, 0] = jnp.where(lower, mix, jnp.where(upper, -flip, 0.0))
        out[0, 0, 0, 1] = jnp.where(lower, flip, mix)


def call(kernel, shapes, *operands, scalars=(), outside=(), scratch=()):
    def space(at):
        return pltpu.SMEM if at in scalars else pltpu.HBM if at in outside else pltpu.VMEM

    out = [jax.ShapeDtypeStruct(shape, jnp.float32) for shape in shapes]
    return pl.pallas_call(
        kernel,
        out_shape=out,
        in_specs=[pl.BlockSpec(memory_space=space(at)) for at in range(len(operands))],
        out_specs=[pl.BlockSpec(memory_space=pltpu.VMEM)] * len(out),
        scratch_shapes=list(scratch),
        compiler_params=pltpu.CompilerParams(vmem_limit_bytes=48 * 2**20),
        cost_estimate=pl.CostEstimate(flops=10**9, bytes_accessed=10**6, transcendentals=0),
    )(*operands)


def first_call(*operands):
    moved = [pltpu.VMEM(operands[at].shape, jnp.float32) for at in (0, 1, 2, 4, 5)]
    return call(
        isolated_kernel, [(2, FULL, 2 * FULL)], *operands, scalars=(3,), outside=(0, 1, 2, 4, 5),
        scratch=moved + [pltpu.SemaphoreType.DMA((5,))],
    )[0]


def permuted(value, pairs):
    return lax.ppermute(value, "dom", pairs)


def on_device(
    hamiltonian, coupling, contact_rates, occupation, lesser_in, greater_in, phonon_shift
):
    count = lax.axis_size("energy")
    swap1 = [(b, b ^ 1) for b in range(8)]
    swap2 = [(b, b ^ 2) for b in range(8)]
    mirror = [(b, b ^ 6) for b in range(8)]
    c_other = permuted(coupling, swap1)
    c_before = permuted(coupling, [(b, b + 1) for b in (1, 3, 5)])
    c_before2 = permuted(coupling, [(b, b + 2) for b in (1, 3, 5)])
    port2 = (2, FULL, 2 * FULL)
    state = (FULL + HALF, 3 * FULL)
    own = first_call(
        hamiltonian, coupling, contact_rates, occupation, lesser_in, greater_in
    )
    g, k, message, middle = call(
        pair_kernel, [state, state, port2, (1, HALF, HALF)],
        coupling, c_other, c_before, c_before2, own, permuted(own, swap1),
    )
    middle_other = permuted(middle, [(2, 0), (3, 1), (4, 6), (5, 7)])
    g, k, message = call(
        quad_kernel, [state, state, (2, HALF, FULL)],
        middle, middle_other, g, k, permuted(message, swap2),
    )
    payload = call(final_kernel, [(2, FULL, FULL)], g, k, permuted(message, mirror))[0]

    def shifted(steps):
        ups = [(e, e + steps) for e in range(count - steps)]
        downs = [(e + steps, e) for e in range(count - steps)]

        def branch(above, below):
            return lax.ppermute(above, "energy", downs), lax.ppermute(below, "energy", ups)

        return branch if steps else lambda above, below: (above, below)

    amount = jnp.clip(phonon_shift[0], 0, quantum_bound - 1)
    above, below = lax.switch(
        amount % fine, [shifted(steps) for steps in range(fine)], payload, payload
    )
    above, below = lax.switch(
        amount // fine,
        [shifted(min(steps, count)) for steps in range(0, quantum_bound, fine)], above, below
    )
    out = (1, 1, 1, 2, FULL, FULL)
    return tuple(call(scatter_kernel, [out, out], above, below))


def solution(mesh):
    blocks_spec = P(None, "energy", "dom", None, None, None)
    return jax.shard_map(
        on_device,
        mesh=mesh,
        in_specs=(
            P("dom", None, None),
            P("dom", None, None),
            P(),
            P(None, "energy", None),
            blocks_spec,
            blocks_spec,
            P(),
        ),
        out_specs=(blocks_spec, blocks_spec),
        check_vma=False,
    )
```

```python
import functools

import jax
import jax.numpy as jnp
from jax import lax
from jax.experimental import pallas as pl
from jax.experimental.pallas import tpu as pltpu
from jax.sharding import PartitionSpec as P

HALF = 64
FULL = 128
broadening = 0.2
phonon_bose = 0.4
phonon_strength = 0.5
quantum_bound = 32
fine = 3


def iota(shape, axis):
    return lax.broadcasted_iota(jnp.int32, shape, axis)


def halves(x):
    high = x.astype(jnp.bfloat16)
    return high, (x - high.astype(jnp.float32)).astype(jnp.bfloat16)


def three_passes(a, b, contracted):
    count = a.shape[0]
    (a_high, a_low), (b_high, b_low) = halves(a), halves(b)
    dims = (((1,), (contracted,)), ((), ()))
    main = lax.dot_general(rows([a_high, a_low]), b_high, dims, preferred_element_type=jnp.float32)
    rest = lax.dot_general(a_high, b_low, dims, preferred_element_type=jnp.float32)
    return main[:count] + (main[count:] + rest)


def dot(a, b):
    return three_passes(a, b, 0)


def dot_nt(a, b):
    return three_passes(a, b, 1)


def rolled(x):
    return jnp.concatenate([x[:, HALF:], x[:, :HALF]], axis=1)


def blocks(x):
    return [x[:, at:at + FULL] for at in range(0, x.shape[1], FULL)]


def lanes(parts):
    return parts[0] if len(parts) == 1 else jnp.concatenate(parts, axis=1)


def rows(parts):
    return parts[0] if len(parts) == 1 else jnp.concatenate(parts, axis=0)


def times_i(x):
    parts = []
    for block in blocks(x):
        turned = rolled(block)
        parts.append(jnp.where(iota(block.shape, 1) < HALF, -turned, turned))
    return lanes(parts)


def expanded(x):
    twin = times_i(x)
    parts = []
    for at in range(0, x.shape[0], HALF):
        parts += [x[at:at + HALF], twin[at:at + HALF]]
    return rows(parts)


def product(a, b):
    return dot(a, expanded(b))


def product_adjoint(a, b):
    return dot_nt(a, expanded(b))


def unit():
    shape = (HALF, FULL)
    return jnp.where(iota(shape, 0) == iota(shape, 1), 1.0, 0.0)


def spread(x, lane):
    at = jnp.full(x.shape, lane, jnp.int32)
    return jnp.take_along_axis(x, at, axis=1, mode="promise_in_bounds")


def panel_of(near, half, k):
    row4, lane4 = iota((4, FULL), 0), iota((4, FULL), 1)
    near_re = [spread(near, k + j) for j in range(4)]
    near_im = [spread(near, HALF + k + j) for j in range(4)]
    piv_re = [c[half:half + 4] for c in near_re]
    piv_im = [c[half:half + 4] for c in near_im]
    local = lane4 & (HALF - 1)
    ones = jnp.where(lane4 == row4 + k, 1.0, 0.0)
    panel = jnp.where((local >= k) & (local < k + 4), ones, near[half:half + 4])
    twin = times_i(panel)
    for j in range(4):
        p_re, p_im = piv_re[j][j:j + 1], piv_im[j][j:j + 1]
        scale = 1.0 / (p_re * p_re + p_im * p_im)
        q_re, q_im = p_re * scale, -(p_im * scale)
        r, t = panel[j:j + 1], twin[j:j + 1]
        new_r = q_re * r + q_im * t
        new_t = q_re * t - q_im * r
        f_re, f_im = piv_re[j], piv_im[j]
        mine = row4 == j
        panel = jnp.where(mine, new_r, panel - (f_re * new_r + f_im * new_t))
        twin = jnp.where(mine, new_t, twin - (f_re * new_t - f_im * new_r))
        for l in range(j + 1, 4):
            u, v = piv_re[l][j:j + 1], piv_im[l][j:j + 1]
            s_re = q_re * u - q_im * v
            s_im = q_re * v + q_im * u
            piv_re[l] = jnp.where(mine, s_re, piv_re[l] - (f_re * s_re - f_im * s_im))
            piv_im[l] = jnp.where(mine, s_im, piv_im[l] - (f_re * s_im + f_im * s_re))
    return panel, twin, near_re, near_im


def cleared(x, re, im, panel, twin, k):
    lane = iota(x.shape, 1) & (HALF - 1)
    x = jnp.where((lane >= k) & (lane < k + 4), 0.0, x)
    for j in range(4):
        x = x - (re[j] * panel[j:j + 1] + im[j] * twin[j:j + 1])
    return x


def inverse(a, work):
    work[...] = a

    def step(block, carry):
        start = pl.multiple_of(block * 8, 8)
        near, a = work[pl.ds(start, 8), :], work[...]
        for half in (0, 4):
            k = start + half
            panel, twin, near_re, near_im = panel_of(near, half, k)
            if half == 0:
                near = cleared(near, near_re, near_im, panel, twin, k)
                near = rows([panel, near[4:]])
            re = [spread(a, k + j) for j in range(4)]
            im = [spread(a, HALF + k + j) for j in range(4)]
            rest = cleared(a, re, im, panel, twin, k)
            row = iota((HALF, FULL), 0)
            both = rows([panel, panel] * 8)
            a = jnp.where((row >= k) & (row < k + 4), both, rest)
        work[...] = a
        return carry

    lax.fori_loop(0, HALF // 8, step, 0)
    return work[...]


def inverse_full(a, work):
    left, right = blocks(a)
    first = inverse(left[:HALF], work)
    below = product(left[HALF:], first)
    last = inverse(right[HALF:] - product(below, right[:HALF]), work)
    ahead = product(first, right[:HALF])
    edges = product(rows([ahead]), last)
    low = -product(last, below)
    top = first + product(edges, below)
    return lanes([rows([top, low]), rows([-edges, last])])


def resolved(sigma_g, work):
    return inverse(unit() - sigma_g, work)


def updated(phi, f, sigma, extra, k_in, kh_in, k_nn, kh_nn, g_row, gh_row, k_row, kh_row, g0, k0):
    count, width = f.shape[0], g_row.shape[1]
    both = 2 * width
    ends = sigma if extra is None else rows([sigma, extra])
    ahead = product(ends, lanes([g_row, k_row, k_nn]))
    x, side = ahead[:HALF, :both], ahead[:HALF, both:]
    inflow = k_in
    if extra is not None:
        g0 = rows([g0[:FULL], g0[FULL:] + ahead[HALF:, :width]])
        k0 = rows([k0[:FULL], k0[FULL:] + ahead[HALF:, width:both]])
        inflow = rows([k_in[:FULL], k_in[FULL:] + ahead[HALF:, both:]])
        x = x + lanes([gh_row, kh_row])
    back = product_adjoint(rows([inflow, side]), ends)
    outflow, kappa = back[:count, :FULL], back[count:, :FULL] + kh_nn
    if extra is not None:
        outflow = rows([outflow[:FULL], outflow[FULL:] + kh_in])
        k0 = lanes([k0[:, :2 * FULL], k0[:, 2 * FULL:] + back[:count, FULL:]])
        x = lanes([x[:, :both - FULL], x[:, both - FULL:] + back[count:, FULL:]])
    u = product(f, phi)
    after = product(u, lanes([x, kappa]))
    g = g0 + after[:, :width]
    k = k0 + after[:, width:both] + product_adjoint(outflow + after[:, both:], u)
    return g, k


def packed_columns(re, im):
    first = iota(re.shape, 1) < HALF
    return lanes([jnp.where(first, re, rolled(im)), jnp.where(first, rolled(re), im)])


def planes(x):
    left, right = blocks(x)
    first = iota(left.shape, 1) < HALF
    return jnp.where(first, left, rolled(right)), jnp.where(first, rolled(left), right)


def flipped(flag, x):
    turned = rows([x[HALF:], x[:HALF]])
    left, right = blocks(turned)
    return jnp.where(flag, lanes([right, left]), x)


def adjoint(x):
    turned = x.T
    return lanes([turned[:HALF], -turned[HALF:]])


def message_of(out_ref, g, k):
    (gf, gn), (kf, kn) = blocks(g), blocks(k)
    row, lane = iota((HALF, FULL), 0), iota((HALF, FULL), 1)
    low = row > (lane & (HALF - 1))
    far, near = kf[:HALF], kn[HALF:]
    out_ref[0], out_ref[1], out_ref[2], out_ref[3] = gf[:HALF], gn[:HALF], gf[HALF:], gn[HALF:]
    out_ref[4] = kn[:HALF]
    out_ref[5] = jnp.where(
        lane < HALF, jnp.where(low, far, rolled(far)), jnp.where(low, rolled(near), near)
    )


def message_from(ref):
    packed = ref[5]
    row, lane = iota((HALF, FULL), 0), iota((HALF, FULL), 1)
    column = lane & (HALF - 1)
    turned = packed.T
    back = rolled(packed)
    ends = []
    for value, flip in (
        (jnp.where(lane < HALF, packed, back), turned[:HALF]),
        (jnp.where(lane < HALF, back, packed), turned[HALF:]),
    ):
        flip = lanes([flip, flip])
        re = jnp.where(row > column, value, jnp.where(row < column, -flip, 0.0))
        im = jnp.where(row > column, flip, value)
        ends.append(jnp.where(lane < HALF, re, im))
    across = ref[4]
    g = rows([lanes([ref[0], ref[1]]), lanes([ref[2], ref[3]])])
    k = rows([lanes([ends[0], across]), lanes([-adjoint(across), ends[1]])])
    return g, k


def isolated_kernel(h_hbm, c_hbm, rates_hbm, occ_ref, lesser_hbm, greater_hbm, out_ref, message_ref,
                    work, h_ref, c_ref, rates_ref, lesser_ref, greater_ref, sems):
    moves = [
        pltpu.make_async_copy(source, target, sems.at[at])
        for at, (source, target) in enumerate((
            (lesser_hbm, lesser_ref), (greater_hbm, greater_ref), (h_hbm, h_ref),
            (c_hbm, c_ref), (rates_hbm, rates_ref),
        ))
    ]
    for move in moves:
        move.start()
    for move in moves:
        move.wait()
    isolated(h_ref, c_ref, rates_ref, occ_ref, lesser_ref, greater_ref, out_ref, message_ref, work)


def isolated(h_ref, c_ref, rates_ref, occ_ref, lesser_ref, greater_ref, out_ref, message_ref, work):
    dom = lax.axis_index("dom")
    energy = lax.axis_index("energy")
    energies = lax.axis_size("energy")
    odd = dom % 2 == 1
    at_left = jnp.where(dom == 0, 1.0, 0.0)
    at_right = jnp.where(dom == lax.axis_size("dom") - 1, 1.0, 0.0)
    shape = (FULL, FULL)
    h = h_ref[0]
    lesser_re, lesser_im = lesser_ref[0, 0, 0, 0], lesser_ref[0, 0, 0, 1]
    greater_re, greater_im = greater_ref[0, 0, 0, 0], greater_ref[0, 0, 0, 1]
    diagonal = iota(shape, 0) == iota(shape, 1)
    index = jnp.full(shape, energy, jnp.int32).astype(jnp.float32)
    value = -1.5 + 3.0 * index / (energies - 1)
    left_rates = lanes([rates_ref[0:1], jnp.zeros((1, HALF), jnp.float32)])
    gamma_left = jnp.where(diagonal, left_rates, 0.0)
    c = c_ref[0]
    corner = dot_nt(c * rates_ref[1:2], c)
    zero = jnp.zeros((HALF, HALF), jnp.float32)
    gamma_right = rows([jnp.zeros((HALF, FULL), jnp.float32), lanes([zero, corner])])
    re = jnp.where(diagonal, value, 0.0) - 0.5 * (h + h.T) - 0.5 * (greater_re - lesser_re)
    im = jnp.where(diagonal, broadening, 0.0) - 0.5 * (greater_im - lesser_im)
    im = im + (0.5 * at_left) * gamma_left + (0.5 * at_right) * gamma_right
    source_im = (
        lesser_im
        + (at_left * occ_ref[0, 0, 0]) * gamma_left
        + (at_right * occ_ref[0, 0, 1]) * gamma_right
    )
    g = inverse_full(flipped(odd, packed_columns(re, im)), work)
    source = flipped(odd, packed_columns(lesser_re, source_im))
    k = product_adjoint(product(g, source), g)
    out_ref[0], out_ref[1] = g, k
    message_of(message_ref, g, k)


def pair_kernel(c_ref, c_other_ref, c_before_ref, c_before2_ref, own_ref, other_ref,
                g_out, k_out, message_out, middle_out, work):
    dom = lax.axis_index("dom")
    odd = dom % 2 == 1
    place = dom // 2
    side = place % 2
    c, c_other = c_ref[0], c_other_ref[0]
    tau = jnp.where(odd, c_other.T, c)
    g, k = own_ref[0], own_ref[1]
    gp, kp = message_from(other_ref)
    (gf, gn), (kf, kn) = blocks(g), blocks(k)
    (gpf, gpn), (kpf, kpn) = blocks(gp), blocks(kp)
    tau_pair = real_pair(tau)
    tall_g = dot(tau, gp[HALF:])
    sides_g = dot_nt(rows([tall_g[:, FULL:], gpn[:HALF]]), tau_pair)
    sigma, gh_fn, gh_nf = sides_g[:HALF], sides_g[HALF:], tall_g[:, :FULL]
    tall_k = dot(tau, kp[HALF:])
    sides_k = dot_nt(rows([tall_k[:, FULL:], kpn[:HALF]]), tau_pair)
    sigma_k, kh_fn, kh_nf = sides_k[:HALF], sides_k[HALF:], tall_k[:, :FULL]
    g_nn, k_nn = gn[HALF:], kn[HALF:]
    mixed = product(rows([sigma, gh_fn]), g_nn)
    phi = resolved(mixed[:HALF], work)
    f = rows([gn, mixed[HALF:]])
    zero = jnp.zeros((HALF, FULL), jnp.float32)
    zero2 = lanes([zero, zero])
    k_in = rows([kn, zero])
    g0 = rows([lanes([g, jnp.zeros((FULL, FULL), jnp.float32)]), lanes([zero2, gpf[:HALF]])])
    k0 = rows([lanes([k, jnp.zeros((FULL, FULL), jnp.float32)]), lanes([zero2, kpf[:HALF]])])
    g1, k1 = updated(
        phi, f, sigma, gh_fn, k_in, kh_fn, k_nn, sigma_k,
        lanes([g[HALF:], zero]), lanes([zero2, gh_nf]),
        lanes([k[HALF:], zero]), lanes([zero2, kh_nf]), g0, k0,
    )
    g_out[...] = g1
    k_out[...] = k1
    last = jnp.where(odd, c, c_other)
    before = jnp.where(odd, c_before2_ref[0], c_before_ref[0])
    kappa = jnp.where(side == 1, before, last.T)
    middle_out[0] = jnp.where(place == 1, last, before)
    ports = []
    for x in (g1, k1):
        b0, _, b2 = blocks(x)
        pair = rows([lanes([b0[:HALF], b2[:HALF]]), lanes([b0[FULL:], b2[FULL:]])])
        pair = flipped(odd != (side == 1), pair)
        pf, pn = blocks(pair)
        tall = dot(kappa, pair[HALF:])
        wide = dot_nt(rows([pn[:HALF], tall[:, FULL:]]), real_pair(kappa))
        ports.append(lanes([rows([pf[:HALF], tall[:, :FULL]]), wide]))
    message_of(message_out, *ports)


def real_pair(tau):
    zero = jnp.zeros_like(tau)
    return rows([lanes([tau, zero]), lanes([zero, tau])])


def quad_kernel(middle_own_ref, middle_other_ref, g_ref, k_ref, other_ref,
                g_out, k_out, message_out, work):
    dom = lax.axis_index("dom")
    odd = dom % 2 == 1
    place = dom // 2
    side = place % 2
    edge = (place == 0) | (place == 3)
    outer = odd == (side == 1)
    g, k = g_ref[...], k_ref[...]
    gp, kp = message_from(other_ref)

    def near_far_columns(x):
        b0, _, b2 = blocks(x)
        return jnp.where(outer, b2, b0), jnp.where(outer, b0, b2)

    def near_far_rows(x):
        return jnp.where(outer, x[FULL:], x[:HALF]), jnp.where(outer, x[:HALF], x[FULL:])

    gc_n, gc_f = near_far_columns(g)
    kc_n, kc_f = near_far_columns(k)
    gr_n, gr_f = near_far_rows(g)
    kr_n, kr_f = near_far_rows(k)
    g_nn, g_fn = near_far_rows(gc_n)
    k_nn, k_fn = near_far_rows(kc_n)
    g_nf, g_ff = near_far_rows(gc_f)
    k_nf, k_ff = near_far_rows(kc_f)
    gpf, gpn = blocks(gp)
    kpf, kpn = blocks(kp)
    sigma, sigma_k = gpn[HALF:], kpn[HALF:]
    gh_fn, kh_fn = gpn[:HALF], kpn[:HALF]
    mixed = product(gpn, g_nn)
    phi = resolved(mixed[HALF:], work)
    zero = jnp.zeros((HALF, FULL), jnp.float32)
    f = rows([gc_n[:FULL], jnp.where(edge, mixed[:HALF], g_fn)])
    k_in = rows([kc_n[:FULL], jnp.where(edge, 0.0, k_fn)])
    zero2 = lanes([zero, zero])

    def row(own, own_q, other_q):
        return lanes([own, jnp.where(edge, 0.0, own_q)]), lanes([zero2, jnp.where(edge, other_q, 0.0)])

    g_row, gh_row = row(gr_n[:, :2 * FULL], g_nf, gpf[HALF:])
    k_row, kh_row = row(kr_n[:, :2 * FULL], k_nf, kpf[HALF:])

    def base(x, x_mf, x_fm, x_ff, other_ff):
        top = lanes([x[:FULL, :2 * FULL], jnp.where(edge, 0.0, x_mf)])
        low = lanes([jnp.where(edge, 0.0, x_fm), jnp.where(edge, other_ff, x_ff)])
        return rows([top, low])

    g2, k2 = updated(
        phi, f, sigma, jnp.where(edge, gh_fn, 0.0), k_in, jnp.where(edge, kh_fn, 0.0), k_nn, sigma_k,
        g_row, gh_row, k_row, kh_row,
        base(g, gc_f[:FULL], gr_f[:, :2 * FULL], g_ff, gpf[:HALF]),
        base(k, kc_f[:FULL], kr_f[:, :2 * FULL], k_ff, kpf[:HALF]),
    )
    g_out[...] = g2
    k_out[...] = k2
    middle = jnp.where(edge, middle_other_ref[0], middle_own_ref[0])
    kappa = jnp.where(place < 2, middle.T, middle)
    tall = dot(kappa, lanes([g2[FULL:, 2 * FULL:], k2[FULL:, 2 * FULL:]]))
    wide = dot_nt(rows(blocks(tall)), real_pair(kappa))
    message_out[0] = wide[:HALF]
    message_out[1] = wide[HALF:]


def final_kernel(g_ref, k_ref, other_ref, out_ref, work):
    odd = lax.axis_index("dom") % 2 == 1
    g, k = g_ref[...], k_ref[...]
    sigma, sigma_k = other_ref[0], other_ref[1]
    g_mn, k_mn = g[:FULL, 2 * FULL:], k[:FULL, 2 * FULL:]
    g_nn, k_nn = g[FULL:, 2 * FULL:], k[FULL:, 2 * FULL:]
    phi = resolved(product(sigma, g_nn), work)
    g3, k3 = updated(
        phi, g_mn, sigma, None, k_mn, None, k_nn, sigma_k,
        g[FULL:, :2 * FULL], None, k[FULL:, :2 * FULL], None,
        g[:FULL, :2 * FULL], k[:FULL, :2 * FULL],
    )
    g_re, g_im = planes(flipped(odd, g3))
    k_re, k_im = planes(flipped(odd, k3))
    lower = iota((FULL, FULL), 0) > iota((FULL, FULL), 1)
    out_ref[0] = jnp.where(lower, k_re, k_im)
    out_ref[1] = jnp.where(lower, k_re + g_re - g_re.T, k_im + g_im + g_im.T)


def scatter_kernel(above_ref, below_ref, lesser_ref, greater_ref, _):
    shape = (FULL, FULL)
    lower = iota(shape, 0) > iota(shape, 1)
    upper = iota(shape, 0) < iota(shape, 1)
    strong = phonon_strength * (phonon_bose + 1.0)
    weak = phonon_strength * phonon_bose
    mixes = (
        strong * above_ref[0] + weak * below_ref[0],
        strong * below_ref[1] + weak * above_ref[1],
    )
    for mix, out in zip(mixes, (lesser_ref, greater_ref)):
        flip = mix.T
        out[0, 0, 0, 0] = jnp.where(lower, mix, jnp.where(upper, -flip, 0.0))
        out[0, 0, 0, 1] = jnp.where(lower, flip, mix)


def call(kernel, shapes, *operands, scalars=(), outside=(), scratch=()):
    def space(at):
        return pltpu.SMEM if at in scalars else pltpu.HBM if at in outside else pltpu.VMEM

    out = [jax.ShapeDtypeStruct(shape, jnp.float32) for shape in shapes]
    return pl.pallas_call(
        kernel,
        out_shape=out,
        in_specs=[pl.BlockSpec(memory_space=space(at)) for at in range(len(operands))],
        out_specs=[pl.BlockSpec(memory_space=pltpu.VMEM)] * len(out),
        scratch_shapes=[pltpu.VMEM((HALF, FULL), jnp.float32), *scratch],
        compiler_params=None if outside else pltpu.CompilerParams(vmem_limit_bytes=48 * 2**20),
        cost_estimate=pl.CostEstimate(flops=10**9, bytes_accessed=10**6, transcendentals=0),
    )(*operands)


def first_call(*operands):
    moved = [pltpu.VMEM(operands[at].shape, jnp.float32) for at in (0, 1, 2, 4, 5)]
    return call(
        isolated_kernel, [(2, FULL, 2 * FULL), (6, HALF, FULL)], *operands, scalars=(3,),
        outside=(0, 1, 2, 4, 5), scratch=moved + [pltpu.SemaphoreType.DMA((5,))],
    )


def permuted(value, pairs):
    return lax.ppermute(value, "dom", pairs)


def on_device(
    hamiltonian, coupling, contact_rates, occupation, lesser_in, greater_in, phonon_shift
):
    count = lax.axis_size("energy")
    swap1 = [(b, b ^ 1) for b in range(8)]
    swap2 = [(b, b ^ 2) for b in range(8)]
    mirror = [(b, b ^ 6) for b in range(8)]
    c_other = permuted(coupling, swap1)
    c_before = permuted(coupling, [(b, b + 1) for b in (1, 3, 5)])
    c_before2 = permuted(coupling, [(b, b + 2) for b in (1, 3, 5)])
    port2 = (6, HALF, FULL)
    state = (FULL + HALF, 3 * FULL)
    own, message = first_call(
        hamiltonian, coupling, contact_rates, occupation, lesser_in, greater_in
    )
    g, k, message, middle = call(
        pair_kernel, [state, state, port2, (1, HALF, HALF)],
        coupling, c_other, c_before, c_before2, own, permuted(message, swap1),
    )
    middle_other = permuted(middle, [(2, 0), (3, 1), (4, 6), (5, 7)])
    g, k, message = call(
        quad_kernel, [state, state, (2, HALF, FULL)],
        middle, middle_other, g, k, permuted(message, swap2),
    )
    payload = call(final_kernel, [(2, FULL, FULL)], g, k, permuted(message, mirror))[0]

    def shifted(steps):
        ups = [(e, e + steps) for e in range(count - steps)]
        downs = [(e + steps, e) for e in range(count - steps)]

        def branch(above, below):
            return lax.ppermute(above, "energy", downs), lax.ppermute(below, "energy", ups)

        return branch if steps else lambda above, below: (above, below)

    amount = jnp.clip(phonon_shift[0], 0, quantum_bound - 1)
    above, below = lax.switch(
        amount % fine, [shifted(steps) for steps in range(fine)], payload, payload
    )
    above, below = lax.switch(
        amount // fine,
        [shifted(min(steps, count)) for steps in range(0, quantum_bound, fine)], above, below
    )
    out = (1, 1, 1, 2, FULL, FULL)
    return tuple(call(scatter_kernel, [out, out], above, below))


def solution(mesh):
    blocks_spec = P(None, "energy", "dom", None, None, None)
    return jax.shard_map(
        on_device,
        mesh=mesh,
        in_specs=(
            P("dom", None, None),
            P("dom", None, None),
            P(),
            P(None, "energy", None),
            blocks_spec,
            blocks_spec,
            P(),
        ),
        out_specs=(blocks_spec, blocks_spec),
        check_vma=False,
    )
```

```python
import functools

import jax
import jax.numpy as jnp
from jax import lax
from jax.experimental import pallas as pl
from jax.experimental.pallas import tpu as pltpu
from jax.sharding import PartitionSpec as P

HALF = 64
FULL = 128
broadening = 0.2
phonon_bose = 0.4
phonon_strength = 0.5
quantum_bound = 32
fine = 3
direct = (16, 17)


def iota(shape, axis):
    return lax.broadcasted_iota(jnp.int32, shape, axis)


def halves(x):
    high = x.astype(jnp.bfloat16)
    return high, (x - high.astype(jnp.float32)).astype(jnp.bfloat16)


def three_passes(a, b, contracted):
    count = a.shape[0]
    (a_high, a_low), (b_high, b_low) = halves(a), halves(b)
    dims = (((1,), (contracted,)), ((), ()))
    main = lax.dot_general(rows([a_high, a_low]), b_high, dims, preferred_element_type=jnp.float32)
    rest = lax.dot_general(a_high, b_low, dims, preferred_element_type=jnp.float32)
    return main[:count] + (main[count:] + rest)


def dot(a, b):
    return three_passes(a, b, 0)


def dot_nt(a, b):
    return three_passes(a, b, 1)


def rolled(x):
    return jnp.concatenate([x[:, HALF:], x[:, :HALF]], axis=1)


def blocks(x):
    return [x[:, at:at + FULL] for at in range(0, x.shape[1], FULL)]


def lanes(parts):
    return parts[0] if len(parts) == 1 else jnp.concatenate(parts, axis=1)


def rows(parts):
    return parts[0] if len(parts) == 1 else jnp.concatenate(parts, axis=0)


def times_i(x):
    parts = []
    for block in blocks(x):
        turned = rolled(block)
        parts.append(jnp.where(iota(block.shape, 1) < HALF, -turned, turned))
    return lanes(parts)


def expanded(x):
    twin = times_i(x)
    parts = []
    for at in range(0, x.shape[0], HALF):
        parts += [x[at:at + HALF], twin[at:at + HALF]]
    return rows(parts)


def product(a, b):
    return dot(a, expanded(b))


def product_adjoint(a, b):
    return dot_nt(a, expanded(b))


def unit():
    shape = (HALF, FULL)
    return jnp.where(iota(shape, 0) == iota(shape, 1), 1.0, 0.0)


def spread(x, lane):
    at = jnp.full(x.shape, lane, jnp.int32)
    return jnp.take_along_axis(x, at, axis=1, mode="promise_in_bounds")


def panel_of(near, half, k):
    row4, lane4 = iota((4, FULL), 0), iota((4, FULL), 1)
    near_re = [spread(near, k + j) for j in range(4)]
    near_im = [spread(near, HALF + k + j) for j in range(4)]
    piv_re = [c[half:half + 4] for c in near_re]
    piv_im = [c[half:half + 4] for c in near_im]
    local = lane4 & (HALF - 1)
    ones = jnp.where(lane4 == row4 + k, 1.0, 0.0)
    panel = jnp.where((local >= k) & (local < k + 4), ones, near[half:half + 4])
    twin = times_i(panel)
    for j in range(4):
        p_re, p_im = piv_re[j][j:j + 1], piv_im[j][j:j + 1]
        scale = 1.0 / (p_re * p_re + p_im * p_im)
        q_re, q_im = p_re * scale, -(p_im * scale)
        r, t = panel[j:j + 1], twin[j:j + 1]
        new_r = q_re * r + q_im * t
        new_t = q_re * t - q_im * r
        f_re, f_im = piv_re[j], piv_im[j]
        mine = row4 == j
        panel = jnp.where(mine, new_r, panel - (f_re * new_r + f_im * new_t))
        twin = jnp.where(mine, new_t, twin - (f_re * new_t - f_im * new_r))
        for l in range(j + 1, 4):
            u, v = piv_re[l][j:j + 1], piv_im[l][j:j + 1]
            s_re = q_re * u - q_im * v
            s_im = q_re * v + q_im * u
            piv_re[l] = jnp.where(mine, s_re, piv_re[l] - (f_re * s_re - f_im * s_im))
            piv_im[l] = jnp.where(mine, s_im, piv_im[l] - (f_re * s_im + f_im * s_re))
    return panel, twin, near_re, near_im


def cleared(x, re, im, panel, twin, k):
    lane = iota(x.shape, 1) & (HALF - 1)
    x = jnp.where((lane >= k) & (lane < k + 4), 0.0, x)
    for j in range(4):
        x = x - (re[j] * panel[j:j + 1] + im[j] * twin[j:j + 1])
    return x


def inverse(a, work):
    work[...] = a

    def step(block, carry):
        start = pl.multiple_of(block * 8, 8)
        near, a = work[pl.ds(start, 8), :], work[...]
        for half in (0, 4):
            k = start + half
            panel, twin, near_re, near_im = panel_of(near, half, k)
            if half == 0:
                near = cleared(near, near_re, near_im, panel, twin, k)
                near = rows([panel, near[4:]])
            re = [spread(a, k + j) for j in range(4)]
            im = [spread(a, HALF + k + j) for j in range(4)]
            rest = cleared(a, re, im, panel, twin, k)
            row = iota((HALF, FULL), 0)
            both = rows([panel, panel] * 8)
            a = jnp.where((row >= k) & (row < k + 4), both, rest)
        work[...] = a
        return carry

    lax.fori_loop(0, HALF // 8, step, 0)
    return work[...]


def inverse_full(a, work):
    left, right = blocks(a)
    first = inverse(left[:HALF], work)
    below = product(left[HALF:], first)
    last = inverse(right[HALF:] - product(below, right[:HALF]), work)
    ahead = product(first, right[:HALF])
    edges = product(rows([ahead]), last)
    low = -product(last, below)
    top = first + product(edges, below)
    return lanes([rows([top, low]), rows([-edges, last])])


def resolved(sigma_g, work):
    return inverse(unit() - sigma_g, work)


def updated(phi, f, sigma, extra, k_in, kh_in, k_nn, kh_nn, g_row, gh_row, k_row, kh_row, g0, k0):
    count, width = f.shape[0], g_row.shape[1]
    both = 2 * width
    ends = sigma if extra is None else rows([sigma, extra])
    ahead = product(ends, lanes([g_row, k_row, k_nn]))
    x, side = ahead[:HALF, :both], ahead[:HALF, both:]
    inflow = k_in
    if extra is not None:
        g0 = rows([g0[:FULL], g0[FULL:] + ahead[HALF:, :width]])
        k0 = rows([k0[:FULL], k0[FULL:] + ahead[HALF:, width:both]])
        inflow = rows([k_in[:FULL], k_in[FULL:] + ahead[HALF:, both:]])
        x = x + lanes([gh_row, kh_row])
    back = product_adjoint(rows([inflow, side]), ends)
    outflow, kappa = back[:count, :FULL], back[count:, :FULL] + kh_nn
    if extra is not None:
        outflow = rows([outflow[:FULL], outflow[FULL:] + kh_in])
        k0 = lanes([k0[:, :2 * FULL], k0[:, 2 * FULL:] + back[:count, FULL:]])
        x = lanes([x[:, :both - FULL], x[:, both - FULL:] + back[count:, FULL:]])
    u = product(f, phi)
    after = product(u, lanes([x, kappa]))
    g = g0 + after[:, :width]
    k = k0 + after[:, width:both] + product_adjoint(outflow + after[:, both:], u)
    return g, k


def packed_columns(re, im):
    first = iota(re.shape, 1) < HALF
    return lanes([jnp.where(first, re, rolled(im)), jnp.where(first, rolled(re), im)])


def planes(x):
    left, right = blocks(x)
    first = iota(left.shape, 1) < HALF
    return jnp.where(first, left, rolled(right)), jnp.where(first, rolled(left), right)


def flipped(flag, x):
    turned = rows([x[HALF:], x[:HALF]])
    left, right = blocks(turned)
    return jnp.where(flag, lanes([right, left]), x)


def adjoint(x):
    turned = x.T
    return lanes([turned[:HALF], -turned[HALF:]])


def message_of(out_ref, g, k):
    (gf, gn), (kf, kn) = blocks(g), blocks(k)
    row, lane = iota((HALF, FULL), 0), iota((HALF, FULL), 1)
    low = row > (lane & (HALF - 1))
    far, near = kf[:HALF], kn[HALF:]
    out_ref[0], out_ref[1], out_ref[2], out_ref[3] = gf[:HALF], gn[:HALF], gf[HALF:], gn[HALF:]
    out_ref[4] = kn[:HALF]
    out_ref[5] = jnp.where(
        lane < HALF, jnp.where(low, far, rolled(far)), jnp.where(low, rolled(near), near)
    )


def message_from(ref):
    packed = ref[5]
    row, lane = iota((HALF, FULL), 0), iota((HALF, FULL), 1)
    column = lane & (HALF - 1)
    turned = packed.T
    back = rolled(packed)
    ends = []
    for value, flip in (
        (jnp.where(lane < HALF, packed, back), turned[:HALF]),
        (jnp.where(lane < HALF, back, packed), turned[HALF:]),
    ):
        flip = lanes([flip, flip])
        re = jnp.where(row > column, value, jnp.where(row < column, -flip, 0.0))
        im = jnp.where(row > column, flip, value)
        ends.append(jnp.where(lane < HALF, re, im))
    across = ref[4]
    g = rows([lanes([ref[0], ref[1]]), lanes([ref[2], ref[3]])])
    k = rows([lanes([ends[0], across]), lanes([-adjoint(across), ends[1]])])
    return g, k


def isolated_kernel(h_hbm, c_hbm, rates_hbm, occ_ref, lesser_hbm, greater_hbm, out_ref, message_ref,
                    work, h_ref, c_ref, rates_ref, lesser_ref, greater_ref, sems):
    moves = [
        pltpu.make_async_copy(source, target, sems.at[at])
        for at, (source, target) in enumerate((
            (lesser_hbm, lesser_ref), (greater_hbm, greater_ref), (h_hbm, h_ref),
            (c_hbm, c_ref), (rates_hbm, rates_ref),
        ))
    ]
    for move in moves:
        move.start()
    for move in moves:
        move.wait()
    isolated(h_ref, c_ref, rates_ref, occ_ref, lesser_ref, greater_ref, out_ref, message_ref, work)


def isolated(h_ref, c_ref, rates_ref, occ_ref, lesser_ref, greater_ref, out_ref, message_ref, work):
    dom = lax.axis_index("dom")
    energy = lax.axis_index("energy")
    energies = lax.axis_size("energy")
    odd = dom % 2 == 1
    at_left = jnp.where(dom == 0, 1.0, 0.0)
    at_right = jnp.where(dom == lax.axis_size("dom") - 1, 1.0, 0.0)
    shape = (FULL, FULL)
    h = h_ref[0]
    lesser_re, lesser_im = lesser_ref[0, 0, 0, 0], lesser_ref[0, 0, 0, 1]
    greater_re, greater_im = greater_ref[0, 0, 0, 0], greater_ref[0, 0, 0, 1]
    diagonal = iota(shape, 0) == iota(shape, 1)
    index = jnp.full(shape, energy, jnp.int32).astype(jnp.float32)
    value = -1.5 + 3.0 * index / (energies - 1)
    left_rates = lanes([rates_ref[0:1], jnp.zeros((1, HALF), jnp.float32)])
    gamma_left = jnp.where(diagonal, left_rates, 0.0)
    c = c_ref[0]
    corner = dot_nt(c * rates_ref[1:2], c)
    zero = jnp.zeros((HALF, HALF), jnp.float32)
    gamma_right = rows([jnp.zeros((HALF, FULL), jnp.float32), lanes([zero, corner])])
    re = jnp.where(diagonal, value, 0.0) - 0.5 * (h + h.T) - 0.5 * (greater_re - lesser_re)
    im = jnp.where(diagonal, broadening, 0.0) - 0.5 * (greater_im - lesser_im)
    im = im + (0.5 * at_left) * gamma_left + (0.5 * at_right) * gamma_right
    source_im = (
        lesser_im
        + (at_left * occ_ref[0, 0, 0]) * gamma_left
        + (at_right * occ_ref[0, 0, 1]) * gamma_right
    )
    g = inverse_full(flipped(odd, packed_columns(re, im)), work)
    source = flipped(odd, packed_columns(lesser_re, source_im))
    k = product_adjoint(product(g, source), g)
    out_ref[0], out_ref[1] = g, k
    message_of(message_ref, g, k)


def pair_kernel(c_ref, c_other_ref, c_before_ref, c_before2_ref, own_ref, other_ref,
                g_out, k_out, message_out, middle_out, work):
    dom = lax.axis_index("dom")
    odd = dom % 2 == 1
    place = dom // 2
    side = place % 2
    c, c_other = c_ref[0], c_other_ref[0]
    tau = jnp.where(odd, c_other.T, c)
    g, k = own_ref[0], own_ref[1]
    gp, kp = message_from(other_ref)
    (gf, gn), (kf, kn) = blocks(g), blocks(k)
    (gpf, gpn), (kpf, kpn) = blocks(gp), blocks(kp)
    tau_pair = real_pair(tau)
    tall_g = dot(tau, gp[HALF:])
    sides_g = dot_nt(rows([tall_g[:, FULL:], gpn[:HALF]]), tau_pair)
    sigma, gh_fn, gh_nf = sides_g[:HALF], sides_g[HALF:], tall_g[:, :FULL]
    tall_k = dot(tau, kp[HALF:])
    sides_k = dot_nt(rows([tall_k[:, FULL:], kpn[:HALF]]), tau_pair)
    sigma_k, kh_fn, kh_nf = sides_k[:HALF], sides_k[HALF:], tall_k[:, :FULL]
    g_nn, k_nn = gn[HALF:], kn[HALF:]
    mixed = product(rows([sigma, gh_fn]), g_nn)
    phi = resolved(mixed[:HALF], work)
    f = rows([gn, mixed[HALF:]])
    zero = jnp.zeros((HALF, FULL), jnp.float32)
    zero2 = lanes([zero, zero])
    k_in = rows([kn, zero])
    g0 = rows([lanes([g, jnp.zeros((FULL, FULL), jnp.float32)]), lanes([zero2, gpf[:HALF]])])
    k0 = rows([lanes([k, jnp.zeros((FULL, FULL), jnp.float32)]), lanes([zero2, kpf[:HALF]])])
    g1, k1 = updated(
        phi, f, sigma, gh_fn, k_in, kh_fn, k_nn, sigma_k,
        lanes([g[HALF:], zero]), lanes([zero2, gh_nf]),
        lanes([k[HALF:], zero]), lanes([zero2, kh_nf]), g0, k0,
    )
    g_out[...] = g1
    k_out[...] = k1
    last = jnp.where(odd, c, c_other)
    before = jnp.where(odd, c_before2_ref[0], c_before_ref[0])
    kappa = jnp.where(side == 1, before, last.T)
    middle_out[0] = jnp.where(place == 1, last, before)
    ports = []
    for x in (g1, k1):
        b0, _, b2 = blocks(x)
        pair = rows([lanes([b0[:HALF], b2[:HALF]]), lanes([b0[FULL:], b2[FULL:]])])
        pair = flipped(odd != (side == 1), pair)
        pf, pn = blocks(pair)
        tall = dot(kappa, pair[HALF:])
        wide = dot_nt(rows([pn[:HALF], tall[:, FULL:]]), real_pair(kappa))
        ports.append(lanes([rows([pf[:HALF], tall[:, :FULL]]), wide]))
    message_of(message_out, *ports)


def real_pair(tau):
    zero = jnp.zeros_like(tau)
    return rows([lanes([tau, zero]), lanes([zero, tau])])


def quad_kernel(middle_own_ref, middle_other_ref, g_ref, k_ref, other_ref,
                g_out, k_out, message_out, work):
    dom = lax.axis_index("dom")
    odd = dom % 2 == 1
    place = dom // 2
    side = place % 2
    edge = (place == 0) | (place == 3)
    outer = odd == (side == 1)
    g, k = g_ref[...], k_ref[...]
    gp, kp = message_from(other_ref)

    def near_far_columns(x):
        b0, _, b2 = blocks(x)
        return jnp.where(outer, b2, b0), jnp.where(outer, b0, b2)

    def near_far_rows(x):
        return jnp.where(outer, x[FULL:], x[:HALF]), jnp.where(outer, x[:HALF], x[FULL:])

    gc_n, gc_f = near_far_columns(g)
    kc_n, kc_f = near_far_columns(k)
    gr_n, gr_f = near_far_rows(g)
    kr_n, kr_f = near_far_rows(k)
    g_nn, g_fn = near_far_rows(gc_n)
    k_nn, k_fn = near_far_rows(kc_n)
    g_nf, g_ff = near_far_rows(gc_f)
    k_nf, k_ff = near_far_rows(kc_f)
    gpf, gpn = blocks(gp)
    kpf, kpn = blocks(kp)
    sigma, sigma_k = gpn[HALF:], kpn[HALF:]
    gh_fn, kh_fn = gpn[:HALF], kpn[:HALF]
    mixed = product(gpn, g_nn)
    phi = resolved(mixed[HALF:], work)
    zero = jnp.zeros((HALF, FULL), jnp.float32)
    f = rows([gc_n[:FULL], jnp.where(edge, mixed[:HALF], g_fn)])
    k_in = rows([kc_n[:FULL], jnp.where(edge, 0.0, k_fn)])
    zero2 = lanes([zero, zero])

    def row(own, own_q, other_q):
        return lanes([own, jnp.where(edge, 0.0, own_q)]), lanes([zero2, jnp.where(edge, other_q, 0.0)])

    g_row, gh_row = row(gr_n[:, :2 * FULL], g_nf, gpf[HALF:])
    k_row, kh_row = row(kr_n[:, :2 * FULL], k_nf, kpf[HALF:])

    def base(x, x_mf, x_fm, x_ff, other_ff):
        top = lanes([x[:FULL, :2 * FULL], jnp.where(edge, 0.0, x_mf)])
        low = lanes([jnp.where(edge, 0.0, x_fm), jnp.where(edge, other_ff, x_ff)])
        return rows([top, low])

    g2, k2 = updated(
        phi, f, sigma, jnp.where(edge, gh_fn, 0.0), k_in, jnp.where(edge, kh_fn, 0.0), k_nn, sigma_k,
        g_row, gh_row, k_row, kh_row,
        base(g, gc_f[:FULL], gr_f[:, :2 * FULL], g_ff, gpf[:HALF]),
        base(k, kc_f[:FULL], kr_f[:, :2 * FULL], k_ff, kpf[:HALF]),
    )
    g_out[...] = g2
    k_out[...] = k2
    middle = jnp.where(edge, middle_other_ref[0], middle_own_ref[0])
    kappa = jnp.where(place < 2, middle.T, middle)
    tall = dot(kappa, lanes([g2[FULL:, 2 * FULL:], k2[FULL:, 2 * FULL:]]))
    wide = dot_nt(rows(blocks(tall)), real_pair(kappa))
    message_out[0] = wide[:HALF]
    message_out[1] = wide[HALF:]


def final_kernel(g_ref, k_ref, other_ref, out_ref, work):
    odd = lax.axis_index("dom") % 2 == 1
    g, k = g_ref[...], k_ref[...]
    sigma, sigma_k = other_ref[0], other_ref[1]
    g_mn, k_mn = g[:FULL, 2 * FULL:], k[:FULL, 2 * FULL:]
    g_nn, k_nn = g[FULL:, 2 * FULL:], k[FULL:, 2 * FULL:]
    phi = resolved(product(sigma, g_nn), work)
    g3, k3 = updated(
        phi, g_mn, sigma, None, k_mn, None, k_nn, sigma_k,
        g[FULL:, :2 * FULL], None, k[FULL:, :2 * FULL], None,
        g[:FULL, :2 * FULL], k[:FULL, :2 * FULL],
    )
    g_re, g_im = planes(flipped(odd, g3))
    k_re, k_im = planes(flipped(odd, k3))
    lower = iota((FULL, FULL), 0) > iota((FULL, FULL), 1)
    out_ref[0] = jnp.where(lower, k_re, k_im)
    out_ref[1] = jnp.where(lower, k_re + g_re - g_re.T, k_im + g_im + g_im.T)


def scatter_kernel(above_ref, below_ref, lesser_ref, greater_ref, _):
    shape = (FULL, FULL)
    lower = iota(shape, 0) > iota(shape, 1)
    upper = iota(shape, 0) < iota(shape, 1)
    strong = phonon_strength * (phonon_bose + 1.0)
    weak = phonon_strength * phonon_bose
    mixes = (
        strong * above_ref[0] + weak * below_ref[0],
        strong * below_ref[1] + weak * above_ref[1],
    )
    for mix, out in zip(mixes, (lesser_ref, greater_ref)):
        flip = mix.T
        out[0, 0, 0, 0] = jnp.where(lower, mix, jnp.where(upper, -flip, 0.0))
        out[0, 0, 0, 1] = jnp.where(lower, flip, mix)


def call(kernel, shapes, *operands, scalars=(), outside=(), scratch=()):
    def space(at):
        return pltpu.SMEM if at in scalars else pltpu.HBM if at in outside else pltpu.VMEM

    out = [jax.ShapeDtypeStruct(shape, jnp.float32) for shape in shapes]
    return pl.pallas_call(
        kernel,
        out_shape=out,
        in_specs=[pl.BlockSpec(memory_space=space(at)) for at in range(len(operands))],
        out_specs=[pl.BlockSpec(memory_space=pltpu.VMEM)] * len(out),
        scratch_shapes=[pltpu.VMEM((HALF, FULL), jnp.float32), *scratch],
        compiler_params=None if outside else pltpu.CompilerParams(vmem_limit_bytes=48 * 2**20),
        cost_estimate=pl.CostEstimate(flops=10**9, bytes_accessed=10**6, transcendentals=0),
    )(*operands)


def first_call(*operands):
    moved = [pltpu.VMEM(operands[at].shape, jnp.float32) for at in (0, 1, 2, 4, 5)]
    return call(
        isolated_kernel, [(2, FULL, 2 * FULL), (6, HALF, FULL)], *operands, scalars=(3,),
        outside=(0, 1, 2, 4, 5), scratch=moved + [pltpu.SemaphoreType.DMA((5,))],
    )


def permuted(value, pairs):
    return lax.ppermute(value, "dom", pairs)


def on_device(
    hamiltonian, coupling, contact_rates, occupation, lesser_in, greater_in, phonon_shift
):
    count = lax.axis_size("energy")
    swap1 = [(b, b ^ 1) for b in range(8)]
    swap2 = [(b, b ^ 2) for b in range(8)]
    mirror = [(b, b ^ 6) for b in range(8)]
    c_other = permuted(coupling, swap1)
    c_before = permuted(coupling, [(b, b + 1) for b in (1, 3, 5)])
    c_before2 = permuted(coupling, [(b, b + 2) for b in (1, 3, 5)])
    port2 = (6, HALF, FULL)
    state = (FULL + HALF, 3 * FULL)
    own, message = first_call(
        hamiltonian, coupling, contact_rates, occupation, lesser_in, greater_in
    )
    g, k, message, middle = call(
        pair_kernel, [state, state, port2, (1, HALF, HALF)],
        coupling, c_other, c_before, c_before2, own, permuted(message, swap1),
    )
    middle_other = permuted(middle, [(2, 0), (3, 1), (4, 6), (5, 7)])
    g, k, message = call(
        quad_kernel, [state, state, (2, HALF, FULL)],
        middle, middle_other, g, k, permuted(message, swap2),
    )
    payload = call(final_kernel, [(2, FULL, FULL)], g, k, permuted(message, mirror))[0]

    def shifted(steps):
        ups = [(e, e + steps) for e in range(count - steps)]
        downs = [(e + steps, e) for e in range(count - steps)]

        def branch(above, below):
            return lax.ppermute(above, "energy", downs), lax.ppermute(below, "energy", ups)

        return branch if steps else lambda above, below: (above, below)

    amount = jnp.clip(phonon_shift[0], 0, quantum_bound - 1)
    coarse = list(range(0, quantum_bound, fine)) + list(direct)
    first, second = amount % fine, amount // fine
    for at, steps in enumerate(direct):
        first = jnp.where(amount == steps, 0, first)
        second = jnp.where(amount == steps, len(coarse) - len(direct) + at, second)
    above, below = lax.switch(first, [shifted(steps) for steps in range(fine)], payload, payload)
    above, below = lax.switch(
        second, [shifted(min(steps, count)) for steps in coarse], above, below
    )
    out = (1, 1, 1, 2, FULL, FULL)
    return tuple(call(scatter_kernel, [out, out], above, below))


def solution(mesh):
    blocks_spec = P(None, "energy", "dom", None, None, None)
    return jax.shard_map(
        on_device,
        mesh=mesh,
        in_specs=(
            P("dom", None, None),
            P("dom", None, None),
            P(),
            P(None, "energy", None),
            blocks_spec,
            blocks_spec,
            P(),
        ),
        out_specs=(blocks_spec, blocks_spec),
        check_vma=False,
    )
```
